128 devices in a mesh: gx: 16 (over z, y_lo, core), gy: 4 (over x), gz: 2 (over y_hi).
Axes of the slice: x: 4, y: 4 (y_hi: 2, y_lo: 2; y = y_hi * 2 + y_lo), z: 4, core: 2. Of those that a mesh axis runs over, the one named last changes fastest.
Arguments:
- models: float32 [2, 256, 128, 256], P(None, 'gx', 'gy', 'gz'), may hold values from -6 to 6
- targets: float32 [2, 256, 128, 256], P(None, 'gx', 'gy', 'gz'), may hold values from -6 to 6
- weights: float32 [2, 256, 128, 256], P(None, 'gx', 'gy', 'gz'), may hold values from 0.5 to 12, as said below
Outputs:
- updated: float32 [2, 256, 128, 256], P(None, 'gx', 'gy', 'gz')
- applied_last: float32 [2, 256, 128, 256], P(None, 'gx', 'gy', 'gz')
The draws below stay inside these ranges and needn't reach their ends.
Inputs may be any that keep to these rules, and one draw needn't show every extreme that they name: Positive data weights.
All inputs are finite; a program needn't handle non-finite values.
Results may differ from the reference program's by a relative error of at most 0.00016.
Values sent between devices are 32-bit elements; how exact they have to be, the bound alone decides.
No kernel may reach another device: no remote copies, remote signals or barrier semaphores. Data moves between devices by JAX's collectives and lax.ppermute only.
A program may use at most 128 MiB of HBM per device.

```python
import math
import jax
import jax.numpy as jnp
from jax import lax

ITERS = 3
NX = 256
NY = 128
NZ = 256


def draw_weights(key, part):
    base_key = jax.random.fold_in(key, 11)
    base = jnp.exp(jax.random.uniform(base_key, (2, NX, NY, NZ), jnp.float32, math.log(0.5), math.log(4.0)))
    ramp = 1.0 + 2.0 * jnp.arange(NX, dtype=jnp.float32) / max(NX - 1, 1)
    return base * ramp[None, :, None, None]


def levels(stream_key, extent, shards, least, high):
    loudness, own = 1.0, jax.random.fold_in(stream_key, 6)
    for dim, parts in shards:
        heights = jnp.exp(jax.random.uniform(jax.random.fold_in(own, dim), (parts,), jnp.float32, least / len(shards), high / len(shards)))
        loudness = loudness * jnp.repeat(heights, extent[dim] // parts).reshape([-1 if axis == dim else 1 for axis in range(len(extent))])
    return loudness


def normal_values(key, shape, width, reach, shards=(), held_as=jnp.bfloat16):
    drawn = jax.random.normal(key, shape, jnp.float32) * width
    if len(shards) > 0:
        drawn = levels(key, shape, shards, -0.22, 0.18) * drawn
    return jnp.clip(drawn, min=-reach, max=reach).astype(held_as)


def setup_inputs(seed: int = 0) -> dict:
    splits = jax.random.split(jax.random.key(seed), 4)
    models = normal_values(splits[0], (2, NX, NY, NZ), 1.0, 6.0, ((1, 16), (2, 4), (3, 2)), jnp.float32)
    targets = normal_values(splits[1], (2, NX, NY, NZ), 1.0, 6.0, ((1, 16), (2, 4), (3, 2)), jnp.float32)
    weights = draw_weights(jax.random.fold_in(splits[3], 71), 0)
    return dict(models=models, targets=targets, weights=weights)


def central(field, which):
    length = field.shape[which]
    widths = [(1, 1) if k == which else (0, 0) for k in range(3)]
    padded = jnp.pad(field, widths)
    upper = lax.slice_in_dim(padded, 2, length + 2, axis=which)
    lower = lax.slice_in_dim(padded, 0, length, axis=which)
    return 0.5 * (upper - lower)


def laplace(field):
    summed = 6.0 * field
    for which in range(3):
        length = field.shape[which]
        widths = [(1, 1) if k == which else (0, 0) for k in range(3)]
        padded = jnp.pad(field, widths)
        summed = summed - lax.slice_in_dim(padded, 2, length + 2, axis=which) - lax.slice_in_dim(padded, 0, length, axis=which)
    return summed


def vector_cross(first_vec, second_vec):
    return (first_vec[1] * second_vec[2] - first_vec[2] * second_vec[1],
            first_vec[2] * second_vec[0] - first_vec[0] * second_vec[2],
            first_vec[0] * second_vec[1] - first_vec[1] * second_vec[0])


def reference(models, targets, weights):
    current = models
    applied = jnp.zeros_like(models)
    for iteration in range(ITERS):
        first_grad = [central(current[0], k) for k in range(3)]
        second_grad = [central(current[1], k) for k in range(3)]
        crossed = vector_cross(first_grad, second_grad)
        first_flux = vector_cross(second_grad, crossed)
        second_flux = vector_cross(crossed, first_grad)
        first_coupling = -2.0 * (central(first_flux[0], 0) + central(first_flux[1], 1) + central(first_flux[2], 2))
        second_coupling = -2.0 * (central(second_flux[0], 0) + central(second_flux[1], 1) + central(second_flux[2], 2))
        smooth = jnp.stack([laplace(current[0]), laplace(current[1])])
        coupling = jnp.stack([first_coupling, second_coupling])
        gradient = weights * (current - targets) + 1.0 * smooth + 0.05 * coupling
        grad_norm = jnp.sum(gradient * gradient)
        applied = weights * gradient + 1.0 * jnp.stack([laplace(gradient[0]), laplace(gradient[1])])
        curvature = jnp.sum(gradient * applied)
        current = current - (grad_norm / curvature) * gradient
    return (current, applied)
```

```python
import jax
import jax.numpy as jnp
from jax import lax
from jax.experimental import pallas as pl
from jax.experimental.pallas import tpu as pltpu
from jax.sharding import PartitionSpec as P

ALL = ("gx", "gy", "gz")
F32 = jnp.float32
NX, NY, NZ = 16, 32, 128
D, DW = 7, 5
X0, Y0 = 7, 8
XE, YE = NX + 2 * D, 56
GRID_X, GRID_Y = 256, 128
EDGE_ROWS = 224
COUPLE = 0.05 * -2.0 * 0.0625


def lane_ids(rows):
    return lax.broadcasted_iota(jnp.int32, (rows, NZ), 1)


def row_ids(rows):
    return lax.broadcasted_iota(jnp.int32, (rows, NZ), 0)


def face_layers():
    return ((0, D, 0), (1, DW, 2 * D), (2, DW, 2 * (D + DW)))


def pack_faces(c, w, t, xp, xn, yp, yn, z, zp, zn):
    iz = lax.axis_index("gz")
    fields = (c, w, t)
    for f, depth, at in face_layers():
        for layer in range(depth):
            for m in range(2):
                xp[at + 2 * layer + m] = fields[f][m, NX - depth + layer]
                xn[at + 2 * layer + m] = fields[f][m, layer]
    for m in range(2):
        for x in range(NX):
            row = (m * NX + x) * (D + 2 * DW)
            for f, depth in ((0, D), (1, DW), (2, DW)):
                yp[row : row + depth] = fields[f][m, x, NY - depth : NY]
                yn[row : row + depth] = fields[f][m, x, 0:depth]
                row += depth
    lane = lane_ids(NY)
    for m in range(2):
        packed = []
        for f in range(3):
            acc = jnp.zeros((NY, NZ), F32)
            for x in range(NX):
                shift = (8 * x + 8 * (1 - iz)) % NZ
                moved = pltpu.roll(fields[f][m, x], shift, 1)
                acc = jnp.where(lane // 8 == x, moved, acc)
            z[f, m] = acc
            packed.append(acc)
        zp[m] = jnp.where(
            lane < 48,
            pltpu.roll(packed[0], 48, 1),
            jnp.where(lane < 80, pltpu.roll(packed[1], 80, 1), pltpu.roll(packed[2], 112, 1)),
        )
        zn[m] = jnp.where(
            lane < 48,
            packed[0],
            jnp.where(lane < 80, pltpu.roll(packed[1], 48, 1), pltpu.roll(packed[2], 80, 1)),
        )


def xy_pieces():
    row = 0
    for side in range(2):
        for m in range(2):
            for f, depth, at in face_layers():
                for away in range(1, depth):
                    count = depth - away
                    layer = depth - away if side == 0 else away - 1
                    place = X0 - away if side == 0 else X0 + NX - 1 + away
                    yield row, count, side, m, f, at + 2 * layer + m, place
                    row += count


def yz_pieces():
    row = 164
    for m in range(2):
        for f, count in ((0, 6), (1, 4), (2, 4)):
            yield row, count, m, f
            row += count


def xyz_pieces():
    row = 192
    for side in range(2):
        for m in range(2):
            yield row, 6, side, m
            row += 6


def pack_edges(xm, xq, z, zm, zq, yp, yn):
    for row, count, side, m, f, layer, place in xy_pieces():
        face = (xm, xq)[side]
        yp[row : row + count] = face[layer, NY - count : NY]
        yn[row : row + count] = face[layer, 0:count]
    for row, count, m, f in yz_pieces():
        yp[row : row + count] = z[f, m, NY - count : NY]
        yn[row : row + count] = z[f, m, 0:count]
    for row, count, side, m in xyz_pieces():
        face = (zm, zq)[side]
        yp[row : row + count] = face[m, NY - count : NY]
        yn[row : row + count] = face[m, 0:count]
    yp[216:224] = jnp.zeros((8, NZ), F32)
    yn[216:224] = jnp.zeros((8, NZ), F32)


def groups():
    for f, first, count in ((0, 0, 6), (1, 6, 4), (2, 10, 4)):
        for k in range(count):
            yield f, first + k, k, count


def assemble(c, w, t, xm, xq, ym, yq, z, zm, zq, em, eq, fields):
    iz = lax.axis_index("gz")

    def clear(x, carry):
        for field in fields:
            for tile in range(2):
                for m in range(2):
                    field[tile, m, x] = jnp.zeros((YE, NZ), F32)
        return carry

    lax.fori_loop(0, XE, clear, 0)

    def own(x, carry):
        for field, source in zip(fields, (c, w, t)):
            for m in range(2):
                field[0, m, X0 + x, Y0 : Y0 + NY] = source[m, x]
        return carry

    lax.fori_loop(0, NX, own, 0)
    top = Y0 + NY
    for f, depth, at in face_layers():
        for layer in range(depth):
            for m in range(2):
                fields[f][0, m, X0 - depth + layer, Y0:top] = xm[at + 2 * layer + m]
                fields[f][0, m, X0 + NX + layer, Y0:top] = xq[at + 2 * layer + m]
    for m in range(2):
        for x in range(NX):
            row = (m * NX + x) * (D + 2 * DW)
            for f, depth in ((0, D), (1, DW), (2, DW)):
                fields[f][0, m, X0 + x, Y0 - depth : Y0] = ym[row : row + depth]
                fields[f][0, m, X0 + x, top : top + depth] = yq[row : row + depth]
                row += depth
    for row, count, side, m, f, layer, place in xy_pieces():
        fields[f][0, m, place, Y0 - count : Y0] = em[row : row + count]
        fields[f][0, m, place, top : top + count] = eq[row : row + count]

    def keep(rows):
        lane = lane_ids(rows)
        return (lane // 8) == 15 * iz

    keep_all, keep_few = keep(NY), keep(8)

    def unpack(rows, group, mask):
        shift = (2 * NZ - 8 * (group + iz)) % NZ
        return jnp.where(mask, pltpu.roll(rows, shift, 1), 0.0)

    for m in range(2):
        for f in range(3):
            packed = z[f, m]
            for x in range(NX):
                fields[f][1, m, X0 + x, Y0:top] = unpack(packed, x, keep_all)
    for row, count, m, f in yz_pieces():
        low, high = em[row : row + 8], eq[row : row + 8]
        for x in range(NX):
            fields[f][1, m, X0 + x, Y0 - count : Y0] = unpack(low, x, keep_few)[0:count]
            fields[f][1, m, X0 + x, top : top + count] = unpack(high, x, keep_few)[0:count]
    for side in range(2):
        for m in range(2):
            packed = (zm, zq)[side][m]
            for f, group, k, count in groups():
                place = X0 - count + k if side == 0 else X0 + NX + k
                fields[f][1, m, place, Y0:top] = unpack(packed, group, keep_all)
    for row, rows, side, m in xyz_pieces():
        low, high = em[row : row + 8], eq[row : row + 8]
        for f, group, k, count in groups():
            place = X0 - count + k if side == 0 else X0 + NX + k
            fields[f][1, m, place, Y0 - rows : Y0] = unpack(low, group, keep_few)[0:rows]
            fields[f][1, m, place, top : top + rows] = unpack(high, group, keep_few)[0:rows]


def cross(a, b):
    return (
        a[1] * b[2] - a[2] * b[1],
        a[2] * b[0] - a[0] * b[2],
        a[0] * b[1] - a[1] * b[0],
    )


def z_pairs(main, halo, first, last):
    main_up, halo_up = pltpu.roll(main, NZ - 1, 1), pltpu.roll(halo, NZ - 1, 1)
    main_down, halo_down = pltpu.roll(main, 1, 1), pltpu.roll(halo, 1, 1)
    return (
        (jnp.where(last, halo_up, main_up), jnp.where(first, halo_down, main_down)),
        (jnp.where(last, main_up, halo_up), jnp.where(first, main_down, halo_down)),
    )


def gradients(C, W, T, G, Fl, depth):
    ix, iy, iz = lax.axis_index("gx"), lax.axis_index("gy"), lax.axis_index("gz")
    lane = lane_ids(8)
    first, last = lane == 0, lane == NZ - 1
    halo_lanes = (lane // 8) == 15 * iz

    def masks(x, y):
        place = ix * NX + (x - X0)
        inside_x = jnp.logical_and(place >= 0, place < GRID_X).astype(F32)
        row = row_ids(8) + (iy * NY + (y - Y0))
        own = jnp.where(jnp.logical_and(row >= 0, row < GRID_Y), inside_x, 0.0)
        return own, jnp.where(halo_lanes, own, 0.0)

    def flux_at(x, carry):
        for k in range(-(-(NY + 2 * depth + 2) // 8)):
            y = Y0 - depth - 1 + 8 * k
            keep = masks(x, y)
            slope = [[None, None], [None, None]]
            for m in range(2):
                shifted = z_pairs(C[0, m, x, y : y + 8], C[1, m, x, y : y + 8], first, last)
                for tile in range(2):
                    slope[tile][m] = (
                        C[tile, m, x + 1, y : y + 8] - C[tile, m, x - 1, y : y + 8],
                        C[tile, m, x, y + 1 : y + 9] - C[tile, m, x, y - 1 : y + 7],
                        shifted[tile][0] - shifted[tile][1],
                    )
            for tile in range(2):
                a, b = slope[tile]
                crossed = tuple(keep[tile] * v for v in cross(a, b))
                flux = cross(b, crossed) + cross(crossed, a)
                for n in range(6):
                    Fl[tile, n, x, y : y + 8] = flux[n]
        return carry

    lax.fori_loop(X0 - depth - 1, X0 + NX + depth + 1, flux_at, 0)

    def gradient_at(x, carry):
        for k in range(-(-(NY + 2 * depth) // 8)):
            y = Y0 - depth + 8 * k
            here, up, down = slice(y, y + 8), slice(y + 1, y + 9), slice(y - 1, y + 7)
            keep = masks(x, y)
            for m in range(2):
                n = 3 * m
                own = [C[tile, m, x, here] for tile in range(2)]
                around = z_pairs(own[0], own[1], first, last)
                along = z_pairs(Fl[0, n + 2, x, here], Fl[1, n + 2, x, here], first, last)
                for tile in range(2):
                    near = around[tile][0] + around[tile][1]
                    near = near + (C[tile, m, x + 1, here] + C[tile, m, x - 1, here])
                    near = near + (C[tile, m, x, up] + C[tile, m, x, down])
                    spread = along[tile][0] - along[tile][1]
                    spread = spread + (Fl[tile, n, x + 1, here] - Fl[tile, n, x - 1, here])
                    spread = spread + (Fl[tile, n + 1, x, up] - Fl[tile, n + 1, x, down])
                    value = W[tile, m, x, here] * (own[tile] - T[tile, m, x, here])
                    value = value + (6.0 * own[tile] - near) + COUPLE * spread
                    G[tile, m, x, here] = keep[tile] * value
        return carry

    lax.fori_loop(X0 - depth, X0 + NX + depth, gradient_at, 0)


def totals(W, G, applied, sums):
    lane = lane_ids(8)
    first, last = lane == 0, lane == NZ - 1

    def body(x, carry):
        norm, curve = carry
        for k in range(NY // 8):
            y = Y0 + 8 * k
            here, up, down = slice(y, y + 8), slice(y + 1, y + 9), slice(y - 1, y + 7)
            for m in range(2):
                own = G[0, m, x, here]
                above = pltpu.roll(own, NZ - 1, 1)
                above = jnp.where(last, pltpu.roll(G[1, m, x, here], NZ - 1, 1), above)
                near = above + G[0, m, x + 1, here] + G[0, m, x, up]
                if applied is None:
                    near = near + near
                else:
                    below = pltpu.roll(own, 1, 1)
                    below = jnp.where(first, pltpu.roll(G[1, m, x, here], 1, 1), below)
                    near = near + below + G[0, m, x - 1, here] + G[0, m, x, down]
                value = W[0, m, x, here] * own + (6.0 * own - near)
                if applied is not None:
                    applied[m, x - X0, 8 * k : 8 * k + 8] = value
                norm = norm + own * own
                curve = curve + own * value
        return norm, curve

    zero = jnp.zeros((8, NZ), F32)
    norm, curve = lax.fori_loop(X0, X0 + NX, body, (zero, zero))
    norm, curve = jnp.sum(norm), jnp.sum(curve)
    row = jnp.where(lane == 0, norm, jnp.where(lane == 1, curve, 0.0))
    for k in range(sums.shape[0] // 8):
        sums[8 * k : 8 * k + 8] = row


def step_of(gathered):
    column = jnp.sum(gathered[...], axis=0, keepdims=True)
    lane = lane_ids(1)
    norm = jnp.sum(jnp.where(lane == 0, column, 0.0), axis=1, keepdims=True)
    curve = jnp.sum(jnp.where(lane == 1, column, 0.0), axis=1, keepdims=True)
    return jnp.broadcast_to(norm, (8, NZ)) / jnp.broadcast_to(curve, (8, NZ))


def moved(C, G, step, New, depth):
    def body(x, carry):
        for k in range(-(-(NY + 2 * depth) // 8)):
            y = Y0 - depth + 8 * k
            for tile in range(2):
                for m in range(2):
                    here = (tile, m, x, slice(y, y + 8))
                    New[here] = C[here] - step * G[here]
        return carry

    lax.fori_loop(X0 - depth, X0 + NX + depth, body, 0)


def first_step(*refs):
    blocks, (C, W, T, G, sums, Fl) = refs[:12], refs[12:]
    assemble(*blocks, (C, W, T))
    gradients(C, W, T, G, Fl, 5)
    totals(W, G, None, sums)


def next_step(C, W, T, G, gathered, New, Gnew, sums, Fl):
    moved(C, G, step_of(gathered), New, 5)
    gradients(New, W, T, Gnew, Fl, 3)
    totals(W, Gnew, None, sums)


def last_step(C, W, T, G, gathered, current, gradient, applied, sums, New, Gnew, Fl):
    moved(C, G, step_of(gathered), New, 3)
    gradients(New, W, T, Gnew, Fl, 1)
    totals(W, Gnew, applied, sums)

    def body(x, carry):
        for m in range(2):
            current[m, x] = New[0, m, X0 + x, Y0 : Y0 + NY]
            gradient[m, x] = Gnew[0, m, X0 + x, Y0 : Y0 + NY]
        return carry

    lax.fori_loop(0, NX, body, 0)


def finish(current, gradient, gathered, updated):
    step = step_of(gathered)

    def body(x, carry):
        for m in range(2):
            for k in range(NY // 8):
                here = (m, x, slice(8 * k, 8 * k + 8))
                updated[here] = current[here] - step * gradient[here]
        return carry

    lax.fori_loop(0, NX, body, 0)


def call(body, name, outs, scratch=(), **more):
    return pl.pallas_call(
        body,
        out_shape=tuple(jax.ShapeDtypeStruct(s, F32) for s in outs),
        scratch_shapes=[pltpu.VMEM(s, F32) for s in scratch],
        compiler_params=pltpu.CompilerParams(vmem_limit_bytes=48 * 1024 * 1024),
        name=name,
        **more,
    )


def local(models, targets, weights):
    nx, ny = lax.axis_size("gx"), lax.axis_size("gy")
    devices = nx * ny * 2
    block = (2, NX, NY, NZ)
    x_face = (2 * (D + 2 * DW), NY, NZ)
    y_face = (2 * NX * (D + 2 * DW), NZ)
    z_edge = (2, NY, NZ)
    xp, xn, yp, yn, z, zp, zn = call(
        pack_faces, "pack_faces", (x_face, x_face, y_face, y_face, (3, 2, NY, NZ), z_edge, z_edge)
    )(models, weights, targets)
    up_x = [(i, i + 1) for i in range(nx - 1)]
    down_x = [(i + 1, i) for i in range(nx - 1)]
    up_y = [(i, i + 1) for i in range(ny - 1)]
    down_y = [(i + 1, i) for i in range(ny - 1)]
    up_xz = [(2 * i + k, 2 * i + 2 + 1 - k) for i in range(nx - 1) for k in range(2)]
    down_xz = [(2 * i + 2 + k, 2 * i + 1 - k) for i in range(nx - 1) for k in range(2)]
    xm, xq = lax.ppermute(xp, "gx", up_x), lax.ppermute(xn, "gx", down_x)
    ym, yq = lax.ppermute(yp, "gy", up_y), lax.ppermute(yn, "gy", down_y)
    zz = lax.ppermute(z, "gz", [(0, 1), (1, 0)])
    zm, zq = lax.ppermute(zp, ("gx", "gz"), up_xz), lax.ppermute(zn, ("gx", "gz"), down_xz)
    edge = (EDGE_ROWS, NZ)
    ep, en = call(pack_edges, "pack_edges", (edge, edge))(xm, xq, zz, zm, zq)
    em, eq = lax.ppermute(ep, "gy", up_y), lax.ppermute(en, "gy", down_y)

    wide = (2, 2, XE, YE, NZ)
    flux = (2, 6, XE, YE, NZ)
    rows = (devices, NZ)

    def gather(sums):
        return lax.all_to_all(sums, ALL, 0, 0, tiled=True)

    C, W, T, G, sums = call(first_step, "first_step", (wide, wide, wide, wide, rows), (flux,))(
        models, weights, targets, xm, xq, ym, yq, zz, zm, zq, em, eq
    )
    C, G, sums = call(next_step, "next_step", (wide, wide, rows), (flux,))(C, W, T, G, gather(sums))
    current, gradient, applied, sums = call(
        last_step, "last_step", (block, block, block, rows), (wide, wide, flux)
    )(C, W, T, G, gather(sums))
    (updated,) = call(finish, "finish", (block,))(current, gradient, gather(sums))
    return updated, applied


def solution(mesh):
    spec = P(None, "gx", "gy", "gz")
    return jax.shard_map(
        local, mesh=mesh, in_specs=(spec, spec, spec), out_specs=(spec, spec), check_vma=False
    )
```

```python
import jax
import jax.numpy as jnp
from jax import lax
from jax.experimental import pallas as pl
from jax.experimental.pallas import tpu as pltpu
from jax.sharding import PartitionSpec as P


ALL = ("gx", "gy", "gz")
F32 = jnp.float32
NX, NY, NZ = 16, 32, 128
D, DW = 7, 5
X0, Y0 = 7, 8
XE, YE = NX + 2 * D, 56
GRID_X, GRID_Y = 256, 128
EDGE_ROWS = 224
COUPLE = 0.05 * -2.0 * 0.0625


def lane_ids(rows):
    return lax.broadcasted_iota(jnp.int32, (rows, NZ), 1)


def row_ids(rows):
    return lax.broadcasted_iota(jnp.int32, (rows, NZ), 0)


def face_layers():
    return ((0, D, 0), (1, DW, 2 * D), (2, DW, 2 * (D + DW)))


def pack_faces(c, w, t, xp, xn, yp, yn, z, zp, zn):
    iz = lax.axis_index("gz")
    fields = (c, w, t)
    for f, depth, at in face_layers():
        for layer in range(depth):
            for m in range(2):
                xp[at + 2 * layer + m] = fields[f][m, NX - depth + layer]
                xn[at + 2 * layer + m] = fields[f][m, layer]
    for m in range(2):
        for x in range(NX):
            row = (m * NX + x) * (D + 2 * DW)
            for f, depth in ((0, D), (1, DW), (2, DW)):
                yp[row : row + depth] = fields[f][m, x, NY - depth : NY]
                yn[row : row + depth] = fields[f][m, x, 0:depth]
                row += depth
    lane = lane_ids(NY)
    for m in range(2):
        packed = []
        for f in range(3):
            acc = jnp.zeros((NY, NZ), F32)
            for x in range(NX):
                shift = (8 * x + 8 * (1 - iz)) % NZ
                moved = pltpu.roll(fields[f][m, x], shift, 1)
                acc = jnp.where(lane // 8 == x, moved, acc)
            z[f, m] = acc
            packed.append(acc)
        zp[m] = jnp.where(
            lane < 48,
            pltpu.roll(packed[0], 48, 1),
            jnp.where(lane < 80, pltpu.roll(packed[1], 80, 1), pltpu.roll(packed[2], 112, 1)),
        )
        zn[m] = jnp.where(
            lane < 48,
            packed[0],
            jnp.where(lane < 80, pltpu.roll(packed[1], 48, 1), pltpu.roll(packed[2], 80, 1)),
        )


def xy_pieces():
    row = 0
    for side in range(2):
        for m in range(2):
            for f, depth, at in face_layers():
                for away in range(1, depth):
                    count = depth - away
                    layer = depth - away if side == 0 else away - 1
                    place = X0 - away if side == 0 else X0 + NX - 1 + away
                    yield row, count, side, m, f, at + 2 * layer + m, place
                    row += count


def yz_pieces():
    row = 164
    for m in range(2):
        for f, count in ((0, 6), (1, 4), (2, 4)):
            yield row, count, m, f
            row += count


def xyz_pieces():
    row = 192
    for side in range(2):
        for m in range(2):
            yield row, 6, side, m
            row += 6


def pack_edges(xm, xq, z, zm, zq, yp, yn):
    for row, count, side, m, f, layer, place in xy_pieces():
        face = (xm, xq)[side]
        yp[row : row + count] = face[layer, NY - count : NY]
        yn[row : row + count] = face[layer, 0:count]
    for row, count, m, f in yz_pieces():
        yp[row : row + count] = z[f, m, NY - count : NY]
        yn[row : row + count] = z[f, m, 0:count]
    for row, count, side, m in xyz_pieces():
        face = (zm, zq)[side]
        yp[row : row + count] = face[m, NY - count : NY]
        yn[row : row + count] = face[m, 0:count]
    yp[216:224] = jnp.zeros((8, NZ), F32)
    yn[216:224] = jnp.zeros((8, NZ), F32)


def groups():
    for f, first, count in ((0, 0, 6), (1, 6, 4), (2, 10, 4)):
        for k in range(count):
            yield f, first + k, k, count


def place_own(c, w, t, *fields):
    def clear(x, carry):
        for field in fields:
            for tile in range(2):
                for m in range(2):
                    field[tile, m, x] = jnp.zeros((YE, NZ), F32)
        return carry

    lax.fori_loop(0, XE, clear, 0)

    def own(x, carry):
        for field, source in zip(fields, (c, w, t)):
            for m in range(2):
                field[0, m, X0 + x, Y0 : Y0 + NY] = source[m, x]
        return carry

    lax.fori_loop(0, NX, own, 0)


def assemble(xm, xq, ym, yq, z, zm, zq, em, eq, fields):
    iz = lax.axis_index("gz")
    top = Y0 + NY
    for f, depth, at in face_layers():
        for layer in range(depth):
            for m in range(2):
                fields[f][0, m, X0 - depth + layer, Y0:top] = xm[at + 2 * layer + m]
                fields[f][0, m, X0 + NX + layer, Y0:top] = xq[at + 2 * layer + m]
    for m in range(2):
        for x in range(NX):
            row = (m * NX + x) * (D + 2 * DW)
            for f, depth in ((0, D), (1, DW), (2, DW)):
                fields[f][0, m, X0 + x, Y0 - depth : Y0] = ym[row : row + depth]
                fields[f][0, m, X0 + x, top : top + depth] = yq[row : row + depth]
                row += depth
    for row, count, side, m, f, layer, place in xy_pieces():
        fields[f][0, m, place, Y0 - count : Y0] = em[row : row + count]
        fields[f][0, m, place, top : top + count] = eq[row : row + count]

    def keep(rows):
        lane = lane_ids(rows)
        return (lane // 8) == 15 * iz

    keep_all, keep_few = keep(NY), keep(8)

    def unpack(rows, group, mask):
        shift = (2 * NZ - 8 * (group + iz)) % NZ
        return jnp.where(mask, pltpu.roll(rows, shift, 1), 0.0)

    for m in range(2):
        for f in range(3):
            packed = z[f, m]
            for x in range(NX):
                fields[f][1, m, X0 + x, Y0:top] = unpack(packed, x, keep_all)
    for row, count, m, f in yz_pieces():
        low, high = em[row : row + 8], eq[row : row + 8]
        for x in range(NX):
            fields[f][1, m, X0 + x, Y0 - count : Y0] = unpack(low, x, keep_few)[0:count]
            fields[f][1, m, X0 + x, top : top + count] = unpack(high, x, keep_few)[0:count]
    for side in range(2):
        for m in range(2):
            packed = (zm, zq)[side][m]
            for f, group, k, count in groups():
                place = X0 - count + k if side == 0 else X0 + NX + k
                fields[f][1, m, place, Y0:top] = unpack(packed, group, keep_all)
    for row, rows, side, m in xyz_pieces():
        low, high = em[row : row + 8], eq[row : row + 8]
        for f, group, k, count in groups():
            place = X0 - count + k if side == 0 else X0 + NX + k
            fields[f][1, m, place, Y0 - rows : Y0] = unpack(low, group, keep_few)[0:rows]
            fields[f][1, m, place, top : top + rows] = unpack(high, group, keep_few)[0:rows]


def cross(a, b):
    return (
        a[1] * b[2] - a[2] * b[1],
        a[2] * b[0] - a[0] * b[2],
        a[0] * b[1] - a[1] * b[0],
    )


def z_pairs(main, halo, first, last):
    main_up, halo_up = pltpu.roll(main, NZ - 1, 1), pltpu.roll(halo, NZ - 1, 1)
    main_down, halo_down = pltpu.roll(main, 1, 1), pltpu.roll(halo, 1, 1)
    return (
        (jnp.where(last, halo_up, main_up), jnp.where(first, halo_down, main_down)),
        (jnp.where(last, main_up, halo_up), jnp.where(first, main_down, halo_down)),
    )


def gradients(C, W, T, G, Fl, depth):
    ix, iy, iz = lax.axis_index("gx"), lax.axis_index("gy"), lax.axis_index("gz")
    lane = lane_ids(8)
    first, last = lane == 0, lane == NZ - 1
    halo_lanes = (lane // 8) == 15 * iz

    def masks(x, y):
        place = ix * NX + (x - X0)
        inside_x = jnp.logical_and(place >= 0, place < GRID_X).astype(F32)
        row = row_ids(8) + (iy * NY + (y - Y0))
        own = jnp.where(jnp.logical_and(row >= 0, row < GRID_Y), inside_x, 0.0)
        return own, jnp.where(halo_lanes, own, 0.0)

    def flux_at(x, carry):
        for k in range(-(-(NY + 2 * depth + 2) // 8)):
            y = Y0 - depth - 1 + 8 * k
            keep = masks(x, y)
            slope = [[None, None], [None, None]]
            for m in range(2):
                shifted = z_pairs(C[0, m, x, y : y + 8], C[1, m, x, y : y + 8], first, last)
                for tile in range(2):
                    slope[tile][m] = (
                        C[tile, m, x + 1, y : y + 8] - C[tile, m, x - 1, y : y + 8],
                        C[tile, m, x, y + 1 : y + 9] - C[tile, m, x, y - 1 : y + 7],
                        shifted[tile][0] - shifted[tile][1],
                    )
            for tile in range(2):
                a, b = slope[tile]
                crossed = tuple(keep[tile] * v for v in cross(a, b))
                flux = cross(b, crossed) + cross(crossed, a)
                for n in range(6):
                    Fl[tile, n, x, y : y + 8] = flux[n]
        return carry

    lax.fori_loop(X0 - depth - 1, X0 + NX + depth + 1, flux_at, 0)

    def gradient_at(x, carry):
        for k in range(-(-(NY + 2 * depth) // 8)):
            y = Y0 - depth + 8 * k
            here, up, down = slice(y, y + 8), slice(y + 1, y + 9), slice(y - 1, y + 7)
            keep = masks(x, y)
            for m in range(2):
                n = 3 * m
                own = [C[tile, m, x, here] for tile in range(2)]
                around = z_pairs(own[0], own[1], first, last)
                along = z_pairs(Fl[0, n + 2, x, here], Fl[1, n + 2, x, here], first, last)
                for tile in range(2):
                    near = around[tile][0] + around[tile][1]
                    near = near + (C[tile, m, x + 1, here] + C[tile, m, x - 1, here])
                    near = near + (C[tile, m, x, up] + C[tile, m, x, down])
                    spread = along[tile][0] - along[tile][1]
                    spread = spread + (Fl[tile, n, x + 1, here] - Fl[tile, n, x - 1, here])
                    spread = spread + (Fl[tile, n + 1, x, up] - Fl[tile, n + 1, x, down])
                    value = W[tile, m, x, here] * (own[tile] - T[tile, m, x, here])
                    value = value + (6.0 * own[tile] - near) + COUPLE * spread
                    G[tile, m, x, here] = keep[tile] * value
        return carry

    lax.fori_loop(X0 - depth, X0 + NX + depth, gradient_at, 0)


def totals(W, G, applied, sums):
    lane = lane_ids(8)
    first, last = lane == 0, lane == NZ - 1

    def body(x, carry):
        norm, curve = carry
        for k in range(NY // 8):
            y = Y0 + 8 * k
            here, up, down = slice(y, y + 8), slice(y + 1, y + 9), slice(y - 1, y + 7)
            for m in range(2):
                own = G[0, m, x, here]
                above = pltpu.roll(own, NZ - 1, 1)
                above = jnp.where(last, pltpu.roll(G[1, m, x, here], NZ - 1, 1), above)
                near = above + G[0, m, x + 1, here] + G[0, m, x, up]
                if applied is None:
                    near = near + near
                else:
                    below = pltpu.roll(own, 1, 1)
                    below = jnp.where(first, pltpu.roll(G[1, m, x, here], 1, 1), below)
                    near = near + below + G[0, m, x - 1, here] + G[0, m, x, down]
                value = W[0, m, x, here] * own + (6.0 * own - near)
                if applied is not None:
                    applied[m, x - X0, 8 * k : 8 * k + 8] = value
                norm = norm + own * own
                curve = curve + own * value
        return norm, curve

    zero = jnp.zeros((8, NZ), F32)
    norm, curve = lax.fori_loop(X0, X0 + NX, body, (zero, zero))
    norm, curve = jnp.sum(norm), jnp.sum(curve)
    row = jnp.where(lane == 0, norm, jnp.where(lane == 1, curve, 0.0))
    for k in range(sums.shape[0] // 8):
        sums[8 * k : 8 * k + 8] = row


def step_of(gathered):
    column = jnp.sum(gathered[...], axis=0, keepdims=True)
    lane = lane_ids(1)
    norm = jnp.sum(jnp.where(lane == 0, column, 0.0), axis=1, keepdims=True)
    curve = jnp.sum(jnp.where(lane == 1, column, 0.0), axis=1, keepdims=True)
    return jnp.broadcast_to(norm, (8, NZ)) / jnp.broadcast_to(curve, (8, NZ))


def moved(C, G, step, New, depth):
    def body(x, carry):
        for k in range(-(-(NY + 2 * depth) // 8)):
            y = Y0 - depth + 8 * k
            for tile in range(2):
                for m in range(2):
                    here = (tile, m, x, slice(y, y + 8))
                    New[here] = C[here] - step * G[here]
        return carry

    lax.fori_loop(X0 - depth, X0 + NX + depth, body, 0)


def first_step(*refs):
    halos, (C, W, T, G, sums, Fl) = refs[3:12], refs[12:]
    assemble(*halos, (C, W, T))
    gradients(C, W, T, G, Fl, 5)
    totals(W, G, None, sums)


def next_step(C, W, T, G, gathered, New, Gnew, sums, Fl):
    moved(C, G, step_of(gathered), New, 5)
    gradients(New, W, T, Gnew, Fl, 3)
    totals(W, Gnew, None, sums)


def last_step(C, W, T, G, gathered, current, gradient, applied, sums, New, Gnew, Fl):
    moved(C, G, step_of(gathered), New, 3)
    gradients(New, W, T, Gnew, Fl, 1)
    totals(W, Gnew, applied, sums)

    def body(x, carry):
        for m in range(2):
            current[m, x] = New[0, m, X0 + x, Y0 : Y0 + NY]
            gradient[m, x] = Gnew[0, m, X0 + x, Y0 : Y0 + NY]
        return carry

    lax.fori_loop(0, NX, body, 0)


def finish(current, gradient, gathered, updated):
    step = step_of(gathered)

    def body(x, carry):
        for m in range(2):
            for k in range(NY // 8):
                here = (m, x, slice(8 * k, 8 * k + 8))
                updated[here] = current[here] - step * gradient[here]
        return carry

    lax.fori_loop(0, NX, body, 0)


def call(body, outs, scratch=(), mib=2, alias=None):
    return pl.pallas_call(
        body,
        out_shape=tuple(jax.ShapeDtypeStruct(s, F32) for s in outs),
        scratch_shapes=[pltpu.VMEM(s, F32) for s in scratch],
        compiler_params=pltpu.CompilerParams(vmem_limit_bytes=mib * 1024 * 1024),
        input_output_aliases=alias or {},
    )


def local(models, targets, weights):
    nx, ny = lax.axis_size("gx"), lax.axis_size("gy")
    devices = nx * ny * 2
    block = (2, NX, NY, NZ)
    wide = (2, 2, XE, YE, NZ)
    flux = (2, 6, XE, YE, NZ)
    rows = (devices, NZ)
    x_face = (2 * (D + 2 * DW), NY, NZ)
    y_face = (2 * NX * (D + 2 * DW), NZ)
    z_edge = (2, NY, NZ)
    xp, xn, yp, yn, z, zp, zn = call(
        pack_faces, (x_face, x_face, y_face, y_face, (3, 2, NY, NZ), z_edge, z_edge)
    )(models, weights, targets)
    up_x = [(i, i + 1) for i in range(nx - 1)]
    down_x = [(i + 1, i) for i in range(nx - 1)]
    up_y = [(i, i + 1) for i in range(ny - 1)]
    down_y = [(i + 1, i) for i in range(ny - 1)]
    up_xz = [(2 * i + k, 2 * i + 2 + 1 - k) for i in range(nx - 1) for k in range(2)]
    down_xz = [(2 * i + 2 + k, 2 * i + 1 - k) for i in range(nx - 1) for k in range(2)]

    zz = lax.ppermute(z, "gz", [(0, 1), (1, 0)])
    zm = lax.ppermute(zp, ("gx", "gz"), up_xz)
    zq = lax.ppermute(zn, ("gx", "gz"), down_xz)
    ym = lax.ppermute(yp, "gy", up_y)
    yq = lax.ppermute(yn, "gy", down_y)
    xm = lax.ppermute(xp, "gx", up_x)
    xq = lax.ppermute(xn, "gx", down_x)
    C, W, T = call(place_own, (wide, wide, wide))(models, weights, targets)
    edge = (EDGE_ROWS, NZ)
    ep, en = call(pack_edges, (edge, edge))(xm, xq, zz, zm, zq)
    em, eq = lax.ppermute(ep, "gy", up_y), lax.ppermute(en, "gy", down_y)

    def gather(sums):
        return lax.all_to_all(sums, ALL, 0, 0, tiled=True)

    C, W, T, G, sums = call(first_step, (wide, wide, wide, wide, rows), (flux,), 13, {0: 0, 1: 1, 2: 2})(
        C, W, T, xm, xq, ym, yq, zz, zm, zq, em, eq
    )
    C, G, sums = call(next_step, (wide, wide, rows), (flux,), 13)(C, W, T, G, gather(sums))
    current, gradient, applied, sums = call(
        last_step, (block, block, block, rows), (wide, wide, flux), 20
    )(C, W, T, G, gather(sums))
    (updated,) = call(finish, (block,))(current, gradient, gather(sums))
    return updated, applied


def solution(mesh):
    spec = P(None, "gx", "gy", "gz")

    return jax.shard_map(
        local, mesh=mesh, in_specs=(spec, spec, spec), out_specs=(spec, spec), check_vma=False
    )
```

```python
import jax
import jax.numpy as jnp
from jax import lax
from jax.experimental import pallas as pl
from jax.experimental.pallas import tpu as pltpu
from jax.sharding import PartitionSpec as P


ALL = ("gx", "gy", "gz")
F32 = jnp.float32
NX, NY, NZ = 16, 32, 128
D, DW = 7, 5
DEPTHS = (D, DW, DW)
X0, Y0 = 7, 8
XE, YE = NX + 2 * D, 56
TOP = Y0 + NY
GRID_X, GRID_Y = 256, 128
COUPLE = 0.05 * -2.0 * 0.0625
SLOT, TILES = 16, 4
XY_ROWS, EDGE_ROWS = 164, 280


def lane_ids(rows):
    return lax.broadcasted_iota(jnp.int32, (rows, NZ), 1)


def row_ids(rows):
    return lax.broadcasted_iota(jnp.int32, (rows, NZ), 0)


def own_lanes(rows, iz):
    return (lane_ids(rows) % SLOT) // 8 == iz


def highs(axis):
    first = 1 - lax.axis_index(axis) % 2
    return first, 1 - first


def face_layers():
    return ((0, D, 0), (1, DW, 2 * D), (2, DW, 2 * (D + DW)))


def xy_pieces():
    row = 0
    for side in range(2):
        for m in range(2):
            for f, depth, at in face_layers():
                for away in range(1, depth):
                    yield row, depth - away, side, m, f, depth, at, away
                    row += depth - away


def seam_pieces():
    row = XY_ROWS
    for tile in range(TILES):
        for m in range(2):
            for f, count in ((0, 6), (1, 4), (2, 4)):
                yield row, count, tile, m, f
                row += count


def pack(c, w, t, *refs):
    fields, seams, (xa, xb, ya, yb, z, za, zb, sems) = refs[:3], refs[3:6], refs[6:]
    iz = lax.axis_index("gz")
    copies = []
    for f, source in enumerate((c, w, t)):
        for m in range(2):
            copy = pltpu.make_async_copy(
                source.at[m],
                fields[f].at[m, pl.ds(X0, NX), pl.ds(Y0, NY)],
                sems.at[2 * f + m],
            )
            copy.start()
            copies.append(copy)
    for copy in copies:
        copy.wait()
    for high, out in zip(highs("gx"), (xa, xb)):
        for f, depth, at in face_layers():
            start = X0 + high * (NX - depth)
            for layer in range(depth):
                for m in range(2):
                    out[at + 2 * layer + m] = fields[f][m, start + layer, Y0:TOP]
    for high, out in zip(highs("gy"), (ya, yb)):
        for m in range(2):
            for x in range(NX):
                row = (m * NX + x) * sum(DEPTHS)
                for f, depth in enumerate(DEPTHS):
                    start = Y0 + high * (NY - depth)
                    out[row : row + depth] = fields[f][m, X0 + x, pl.ds(start, depth)]
                    row += depth
    lane, own = lane_ids(NY), own_lanes(NY, iz)
    swap = 8 + 112 * iz
    for half in range(2):
        for m in range(2):
            packed = []
            for f in range(3):
                acc = jnp.zeros((NY, NZ), F32)
                for s in range(8):
                    block = fields[f][m, X0 + 8 * half + s, Y0:TOP]
                    turned = pltpu.roll(block, (SLOT * s + 8) % NZ, 1)
                    acc = jnp.where(jnp.logical_and(lane // SLOT == s, own), turned, acc)
                seams[f][m, 1 + half, Y0:TOP] = acc
                packed.append(acc)
            z[half, 0, m] = packed[0] + pltpu.roll(packed[1], swap, 1)
            z[half, 1, m] = packed[2]
    for high, out in zip(highs("gx"), (za, zb)):
        for pair in range(2):
            for m in range(2):
                out[pair, m] = z[high, pair, m]


def clear(*refs):
    fields, seams = refs[6:9], refs[9:12]
    blank = jnp.zeros((YE, NZ), F32)
    for field in fields:
        for m in range(2):
            for x in (*range(X0), *range(X0 + NX, XE)):
                field[m, x] = blank
            for x in range(X0, X0 + NX):
                field[m, x, 0:Y0] = blank[0:Y0]
                field[m, x, TOP:YE] = blank[TOP:YE]
    for seam in seams:
        for m in range(2):
            for tile in (0, 3):
                seam[m, tile] = blank
            for tile in (1, 2):
                seam[m, tile, 0:Y0] = blank[0:Y0]
                seam[m, tile, TOP:YE] = blank[TOP:YE]


def build(xa, xb, z, za, zb, *refs):
    seams, (ea, eb) = refs[3:6], refs[6:]
    iz = lax.axis_index("gz")
    lane, own = lane_ids(NY), own_lanes(NY, iz)
    swap = 8 + 112 * iz

    def others(pairs):
        return pairs[0], pltpu.roll(pairs[0], swap, 1), pairs[1]

    for m in range(2):
        for half in range(2):
            for f, other in enumerate(others([z[half, pair, m] for pair in range(2)])):
                here = (m, 1 + half, slice(Y0, TOP))
                seams[f][here] = jnp.where(own, seams[f][here], other)
    for high, face, edge in zip(highs("gx"), (xa, xb), (za, zb)):
        for m in range(2):
            halves = others([edge[pair, m] for pair in range(2)])
            for f, depth, at in face_layers():
                acc = halves[f]
                for layer in range(depth):
                    s = jnp.where(high == 1, layer, 8 - depth + layer)
                    turned = pltpu.roll(face[at + 2 * layer + m], (SLOT * s + 8) % NZ, 1)
                    acc = jnp.where(jnp.logical_and(lane // SLOT == s, own), turned, acc)
                seams[f][m, 3 * high, Y0:TOP] = acc
    high_x = highs("gx")
    for high, out in zip(highs("gy"), (ea, eb)):
        for row, count, side, m, f, depth, at, away in xy_pieces():
            layer = jnp.where(high_x[side] == 1, away - 1, depth - away)
            start = high * (NY - count)
            out[row : row + count] = (xa, xb)[side][at + 2 * layer + m, pl.ds(start, count)]
        for row, count, tile, m, f in seam_pieces():
            start = Y0 + high * (NY - count)
            out[row : row + count] = seams[f][m, tile, pl.ds(start, count)]
        out[276:280] = jnp.zeros((4, NZ), F32)


def place(xa, xb, ya, yb, *refs):
    fields = refs[3:]
    for high, face in zip(highs("gx"), (xa, xb)):
        for f, depth, at in face_layers():
            start = jnp.where(high == 1, X0 + NX, X0 - depth)
            for layer in range(depth):
                for m in range(2):
                    fields[f][m, start + layer, Y0:TOP] = face[at + 2 * layer + m]
    for high, face in zip(highs("gy"), (ya, yb)):
        for m in range(2):
            for x in range(NX):
                row = (m * NX + x) * sum(DEPTHS)
                for f, depth in enumerate(DEPTHS):
                    start = jnp.where(high == 1, TOP, Y0 - depth)
                    fields[f][m, X0 + x, pl.ds(start, depth)] = face[row : row + depth]
                    row += depth


def place_edges(ea, eb, fields, seams):
    high_x = highs("gx")
    for high, edge in zip(highs("gy"), (ea, eb)):
        for row, count, side, m, f, depth, at, away in xy_pieces():
            x = jnp.where(high_x[side] == 1, X0 + NX - 1 + away, X0 - away)
            start = jnp.where(high == 1, TOP, Y0 - count)
            fields[f][m, x, pl.ds(start, count)] = edge[row : row + count]
        for row, count, tile, m, f in seam_pieces():
            start = jnp.where(high == 1, TOP, Y0 - count)
            seams[f][m, tile, pl.ds(start, count)] = edge[row : row + count]


def cross(a, b):
    return (
        a[1] * b[2] - a[2] * b[1],
        a[2] * b[0] - a[0] * b[2],
        a[0] * b[1] - a[1] * b[0],
    )


class Along:
    def __init__(self):
        iz = lax.axis_index("gz")
        self.iz = iz
        lane = lane_ids(8)
        self.first, self.last = lane == 0, lane == NZ - 1
        self.up_on = (1 - iz).astype(F32)
        self.down_on = iz.astype(F32)

    def slot(self, x):
        place = x + 1
        return place // 8, (119 + 2 * self.iz + NZ - SLOT * (place % 8)) % NZ

    def __call__(self, own, seam, shift):
        over = pltpu.roll(seam, shift, 1)
        up = jnp.where(self.last, over * self.up_on, pltpu.roll(own, NZ - 1, 1))
        down = jnp.where(self.first, over * self.down_on, pltpu.roll(own, 1, 1))
        return up, down


def seam_x(ref, lead, tile, rows):
    lane = lane_ids(8)
    own = ref[(*lead, tile, rows)]
    after = ref[(*lead, min(tile + 1, TILES - 1), rows)]
    before = ref[(*lead, max(tile - 1, 0), rows)]
    up = jnp.where(lane < NZ - SLOT, pltpu.roll(own, NZ - SLOT, 1), pltpu.roll(after, NZ - SLOT, 1))
    down = jnp.where(lane >= SLOT, pltpu.roll(own, SLOT, 1), pltpu.roll(before, SLOT, 1))
    return own, up, down


def chunks(rows):
    return -(-rows // 8)


def seam_gradients(C, W, T, G, Fl, depth):
    ix, iy = lax.axis_index("gx"), lax.axis_index("gy")
    lane = lane_ids(8)

    def keep(tile, y):
        place = ix * NX + (8 * tile - 8) + lane // SLOT
        row = row_ids(8) + (iy * NY - Y0) + y
        inside = jnp.logical_and(place >= 0, place < GRID_X)
        inside = jnp.logical_and(inside, jnp.logical_and(row >= 0, row < GRID_Y))
        return inside.astype(F32)

    def flux_at(k, carry):
        y = Y0 - depth - 1 + 8 * k
        here = pl.ds(y, 8)
        for tile in range(TILES):
            slope = []
            for m in range(2):
                own, after, before = seam_x(C, (m,), tile, here)
                slope.append(
                    (
                        after - before,
                        C[m, tile, pl.ds(y + 1, 8)] - C[m, tile, pl.ds(y - 1, 8)],
                        pltpu.roll(own, NZ - 1, 1) - pltpu.roll(own, 1, 1),
                    )
                )
            a, b = slope
            inside = keep(tile, y)
            crossed = tuple(inside * v for v in cross(a, b))
            for n, value in enumerate(cross(b, crossed) + cross(crossed, a)):
                Fl[n, tile, here] = value
        return carry

    lax.fori_loop(0, chunks(NY + 2 * depth + 2), flux_at, 0)

    def gradient_at(k, carry):
        y = Y0 - depth + 8 * k
        here, up, down = pl.ds(y, 8), pl.ds(y + 1, 8), pl.ds(y - 1, 8)
        for tile in range(TILES):
            inside = keep(tile, y)
            for m in range(2):
                n = 3 * m
                own, after, before = seam_x(C, (m,), tile, here)
                near = after + before + C[m, tile, up] + C[m, tile, down]
                near = near + pltpu.roll(own, NZ - 1, 1) + pltpu.roll(own, 1, 1)
                _, after, before = seam_x(Fl, (n,), tile, here)
                along = Fl[n + 2, tile, here]
                spread = after - before + (Fl[n + 1, tile, up] - Fl[n + 1, tile, down])
                spread = spread + (pltpu.roll(along, NZ - 1, 1) - pltpu.roll(along, 1, 1))
                value = W[m, tile, here] * (own - T[m, tile, here])
                value = value + (6.0 * own - near) + COUPLE * spread
                G[m, tile, here] = inside * value
        return carry

    lax.fori_loop(0, chunks(NY + 2 * depth), gradient_at, 0)


def gradients(fields, seams, G, Gs, Fl, Fs, depth):
    C, W, T = fields
    seam_gradients(*seams, Gs, Fs, depth)
    ix, iy = lax.axis_index("gx"), lax.axis_index("gy")
    along = Along()

    def keep(x, y):
        place = ix * NX + (x - X0)
        inside_x = jnp.logical_and(place >= 0, place < GRID_X).astype(F32)
        row = row_ids(8) + (iy * NY + (y - Y0))
        return jnp.where(jnp.logical_and(row >= 0, row < GRID_Y), inside_x, 0.0)

    def flux_at(x, carry):
        tile, shift = along.slot(x)
        for k in range(chunks(NY + 2 * depth + 2)):
            y = Y0 - depth - 1 + 8 * k
            here, up, down = slice(y, y + 8), slice(y + 1, y + 9), slice(y - 1, y + 7)
            slope, around = [], []
            for m in range(2):
                after, before = along(C[m, x, here], seams[0][m, tile, here], shift)
                slope.append(
                    (
                        C[m, x + 1, here] - C[m, x - 1, here],
                        C[m, x, up] - C[m, x, down],
                        after - before,
                    )
                )
                around.append(after + before)
            a, b = slope
            inside = keep(x, y)
            crossed = tuple(inside * v for v in cross(a, b))
            for m, flux in enumerate((cross(b, crossed), cross(crossed, a))):
                after, before = along(flux[2], Fs[3 * m + 2, tile, here], shift)
                Fl[3 * m, x, here] = flux[0]
                Fl[3 * m + 1, x, here] = flux[1]
                Fl[3 * m + 2, x, here] = COUPLE * (after - before) - around[m]
        return carry

    lax.fori_loop(X0 - depth - 1, X0 + NX + depth + 1, flux_at, 0)

    def gradient_at(x, carry):
        for k in range(chunks(NY + 2 * depth)):
            y = Y0 - depth + 8 * k
            here, up, down = slice(y, y + 8), slice(y + 1, y + 9), slice(y - 1, y + 7)
            inside = keep(x, y)
            for m in range(2):
                n = 3 * m
                own = C[m, x, here]
                near = (C[m, x + 1, here] + C[m, x - 1, here]) + (C[m, x, up] + C[m, x, down])
                spread = Fl[n, x + 1, here] - Fl[n, x - 1, here]
                spread = spread + (Fl[n + 1, x, up] - Fl[n + 1, x, down])
                value = W[m, x, here] * (own - T[m, x, here]) + (6.0 * own - near)
                G[m, x, here] = inside * (value + (Fl[n + 2, x, here] + COUPLE * spread))
        return carry

    lax.fori_loop(X0 - depth, X0 + NX + depth, gradient_at, 0)


def totals(W, G, Gs, applied, sums):
    along = Along()

    def body(x, carry):
        norm, curve = carry
        tile, shift = along.slot(x)
        for k in range(NY // 8):
            y = Y0 + 8 * k
            here, up, down = slice(y, y + 8), slice(y + 1, y + 9), slice(y - 1, y + 7)
            for m in range(2):
                own = G[m, x, here]
                after, before = along(own, Gs[m, tile, here], shift)
                near = after + G[m, x + 1, here] + G[m, x, up]
                if applied is None:
                    near = near + near
                else:
                    near = near + before + G[m, x - 1, here] + G[m, x, down]
                value = W[m, x, here] * own + (6.0 * own - near)
                if applied is not None:
                    applied[m, x - X0, 8 * k : 8 * k + 8] = value
                norm = norm + own * own
                curve = curve + own * value
        return norm, curve

    zero = jnp.zeros((8, NZ), F32)
    norm, curve = lax.fori_loop(X0, X0 + NX, body, (zero, zero))
    norm, curve = jnp.sum(norm), jnp.sum(curve)
    lane = lane_ids(8)
    row = jnp.where(lane == 0, norm, jnp.where(lane == 1, curve, 0.0))
    for k in range(sums.shape[0] // 8):
        sums[8 * k : 8 * k + 8] = row


def step_of(gathered):
    column = jnp.sum(gathered[...], axis=0, keepdims=True)
    lane = lane_ids(1)
    norm = jnp.sum(jnp.where(lane == 0, column, 0.0), axis=1, keepdims=True)
    curve = jnp.sum(jnp.where(lane == 1, column, 0.0), axis=1, keepdims=True)
    return jnp.broadcast_to(norm, (8, NZ)) / jnp.broadcast_to(curve, (8, NZ))


def moved(C, Cs, G, Gs, step, New, News, depth):
    rows = [slice(Y0 - depth + 8 * k, Y0 - depth + 8 * k + 8) for k in range(chunks(NY + 2 * depth))]

    def body(x, carry):
        for here in rows:
            for m in range(2):
                New[m, x, here] = C[m, x, here] - step * G[m, x, here]
        return carry

    lax.fori_loop(X0 - depth, X0 + NX + depth, body, 0)
    for tile in range(TILES):
        for here in rows:
            for m in range(2):
                News[m, tile, here] = Cs[m, tile, here] - step * Gs[m, tile, here]


def first_step(ea, eb, *refs):
    fields, seams, (G, Gs, sums, Fl, Fs) = refs[6:9], refs[9:12], refs[12:]
    place_edges(ea, eb, fields, seams)
    gradients(fields, seams, G, Gs, Fl, Fs, 5)
    totals(fields[1], G, Gs, None, sums)


def next_step(C, W, T, Cs, Ws, Ts, G, Gs, gathered, New, News, Gn, Gns, sums, Fl, Fs):
    moved(C, Cs, G, Gs, step_of(gathered), New, News, 5)
    gradients((New, W, T), (News, Ws, Ts), Gn, Gns, Fl, Fs, 3)
    totals(W, Gn, Gns, None, sums)


def last_step(C, W, T, Cs, Ws, Ts, G, Gs, gathered, *refs):
    current, gradient, applied, sums, New, News, Gn, Gns, Fl, Fs = refs
    moved(C, Cs, G, Gs, step_of(gathered), New, News, 3)
    gradients((New, W, T), (News, Ws, Ts), Gn, Gns, Fl, Fs, 1)
    totals(W, Gn, Gns, applied, sums)

    def body(x, carry):
        for m in range(2):
            current[m, x] = New[m, X0 + x, Y0:TOP]
            gradient[m, x] = Gn[m, X0 + x, Y0:TOP]
        return carry

    lax.fori_loop(0, NX, body, 0)


def finish(current, gradient, gathered, updated):
    step = step_of(gathered)

    def body(x, carry):
        for m in range(2):
            for k in range(NY // 8):
                here = (m, x, slice(8 * k, 8 * k + 8))
                updated[here] = current[here] - step * gradient[here]
        return carry

    lax.fori_loop(0, NX, body, 0)


def call(body, outs, scratch=(), mib=2, alias=None, **more):
    return pl.pallas_call(
        body,
        out_shape=tuple(jax.ShapeDtypeStruct(s, F32) for s in outs),
        scratch_shapes=[pltpu.VMEM(s, F32) if isinstance(s, tuple) else s for s in scratch],
        compiler_params=pltpu.CompilerParams(vmem_limit_bytes=mib * 1024 * 1024),
        input_output_aliases=alias or {},
        **more,
    )


def pairs_of(size):
    first = [(i, i ^ 1) for i in range(size)]
    second = [(i, i - 1 if i % 2 == 0 else i + 1) for i in range(1, size - 1)]
    return first, second


def gather(sums):
    return lax.all_to_all(sums, ALL, 0, 0, tiled=True)


def local(models, targets, weights):
    nx, ny = lax.axis_size("gx"), lax.axis_size("gy")
    block = (2, NX, NY, NZ)
    wide, seam = (2, XE, YE, NZ), (2, TILES, YE, NZ)
    flux = ((6, XE, YE, NZ), (6, TILES, YE, NZ))
    rows = (nx * ny * 2, NZ)
    states = (wide,) * 3 + (seam,) * 3
    x_face, y_face = (2 * sum(DEPTHS), NY, NZ), (2 * NX * sum(DEPTHS), NZ)
    z_half, edge = (2, 2, NY, NZ), (EDGE_ROWS, NZ)
    *state, xa, xb, ya, yb, z, za, zb = call(
        pack,
        (*states, x_face, x_face, y_face, y_face, (2, *z_half), z_half, z_half),
        (pltpu.SemaphoreType.DMA((6,)),),
        in_specs=[pl.BlockSpec(memory_space=pltpu.HBM)] * 3,
    )(models, weights, targets)
    first_x, second_x = pairs_of(nx)
    first_y, second_y = pairs_of(ny)

    def across(pairs):
        return [(2 * i + k, 2 * j + 1 - k) for i, j in pairs for k in range(2)]

    xa, xb = lax.ppermute(xa, "gx", first_x), lax.ppermute(xb, "gx", second_x)
    ya, yb = lax.ppermute(ya, "gy", first_y), lax.ppermute(yb, "gy", second_y)
    z = lax.ppermute(z, "gz", [(0, 1), (1, 0)])
    za = lax.ppermute(za, ("gx", "gz"), across(first_x))
    zb = lax.ppermute(zb, ("gx", "gz"), across(second_x))
    state = call(clear, states, alias={i: i for i in range(6)})(*state)
    *seams, ea, eb = call(build, (seam,) * 3 + (edge, edge), alias={5: 0, 6: 1, 7: 2})(
        xa, xb, z, za, zb, *state[3:]
    )
    ea, eb = lax.ppermute(ea, "gy", first_y), lax.ppermute(eb, "gy", second_y)
    fields = call(place, (wide,) * 3, alias={4: 0, 5: 1, 6: 2})(xa, xb, ya, yb, *state[:3])
    *state, G, Gs, sums = call(
        first_step, (*states, wide, seam, rows), flux, 9, {2 + i: i for i in range(6)}
    )(ea, eb, *fields, *seams)
    C, Cs, G, Gs, sums = call(next_step, (wide, seam, wide, seam, rows), flux, 9)(
        *state, G, Gs, gather(sums)
    )
    state = (C, *state[1:3], Cs, *state[4:])
    current, gradient, applied, sums = call(
        last_step, (block, block, block, rows), (wide, seam, wide, seam, *flux), 14
    )(*state, G, Gs, gather(sums))
    (updated,) = call(finish, (block,))(current, gradient, gather(sums))
    return updated, applied


def solution(mesh):
    spec = P(None, "gx", "gy", "gz")

    return jax.shard_map(
        local, mesh=mesh, in_specs=(spec, spec, spec), out_specs=(spec, spec), check_vma=False
    )
```

```python
import jax
import jax.numpy as jnp
from jax import lax
from jax.experimental import pallas as pl
from jax.experimental.pallas import tpu as pltpu
from jax.sharding import PartitionSpec as P


ALL = ("gx", "gy", "gz")
F32 = jnp.float32
NX, NY, NZ = 16, 32, 128
DEPTHS = (7, 5, 5)
DX = 3
X_DEPTHS = (DX, 1, 1)
X0, Y0 = DX, 8
XE, YE = NX + 2 * DX, 56
TOP = Y0 + NY
GRID_X, GRID_Y = 256, 128
COUPLE = 0.05 * -2.0 * 0.0625
SLOT, TILES = 16, 4
XY_ROWS, EDGE_ROWS = 44, 128
SIDE = slice(Y0 - 4, Y0 + NY + 4)
SIDE_ROWS = NY + 8


def lane_ids(rows):
    return lax.broadcasted_iota(jnp.int32, (rows, NZ), 1)


def row_ids(rows):
    return lax.broadcasted_iota(jnp.int32, (rows, NZ), 0)


def own_lanes(rows, iz):
    return (lane_ids(rows) % SLOT) // 8 == iz


def highs(axis):
    first = 1 - lax.axis_index(axis) % 2
    return first, 1 - first


def face_layers():
    return ((0, DX, 0), (1, 1, 2 * DX), (2, 1, 2 * DX + 2))


def xy_pieces():
    row = 0
    for side in range(2):
        for m in range(2):
            for away in (1, 2):
                yield row, 7 - away, side, m, away
                row += 7 - away


def seam_pieces():
    row = XY_ROWS
    for tile in range(TILES):
        for m in range(2):
            for f, count in ((0, 6), (1, 4), (2, 4)) if tile in (1, 2) else ((0, 6),):
                yield row, count, tile, m, f
                row += count


def pack(c, w, t, *refs):
    fields, seams, (xa, xb, ya, yb, z, za, zb, sems) = refs[:3], refs[3:6], refs[6:]
    iz = lax.axis_index("gz")
    copies = []
    for f, source in enumerate((c, w, t)):
        for m in range(2):
            copy = pltpu.make_async_copy(
                source.at[m],
                fields[f].at[m, pl.ds(X0, NX), pl.ds(Y0, NY)],
                sems.at[2 * f + m],
            )
            copy.start()
            copies.append(copy)
    for copy in copies:
        copy.wait()
    for high, out in zip(highs("gx"), (xa, xb)):
        for f, depth, at in face_layers():
            start = X0 + high * (NX - depth)
            for layer in range(depth):
                for m in range(2):
                    out[at + 2 * layer + m] = fields[f][m, start + layer, Y0:TOP]
    for high, out in zip(highs("gy"), (ya, yb)):
        for m in range(2):
            for x in range(NX):
                row = (m * NX + x) * sum(DEPTHS)
                for f, depth in enumerate(DEPTHS):
                    start = Y0 + high * (NY - depth)
                    out[row : row + depth] = fields[f][m, X0 + x, pl.ds(start, depth)]
                    row += depth
    lane, own = lane_ids(NY), own_lanes(NY, iz)
    swap = 8 + 112 * iz
    edges = []
    for half in range(2):
        models, targets = [], []
        for m in range(2):
            packed = []
            for f in range(3):
                acc = jnp.zeros((NY, NZ), F32)
                for s in range(8):
                    block = fields[f][m, X0 + 8 * half + s, Y0:TOP]
                    turned = pltpu.roll(block, (SLOT * s + 8) % NZ, 1)
                    acc = jnp.where(jnp.logical_and(lane // SLOT == s, own), turned, acc)
                seams[f][m, 1 + half, Y0:TOP] = acc
                packed.append(acc)
            z[half, m] = packed[0] + pltpu.roll(packed[1], swap, 1)
            models.append(packed[0])
            targets.append(packed[2])
        z[half, 2] = targets[0] + pltpu.roll(targets[1], swap, 1)
        edges.append(models[0] + pltpu.roll(models[1], swap, 1))
    for high, out in zip(highs("gx"), (za, zb)):
        out[...] = jnp.where(high == 1, edges[1], edges[0])


def clear(*refs):
    fields, seams = refs[6:9], refs[9:12]
    blank = jnp.zeros((YE, NZ), F32)
    for field in fields:
        for m in range(2):
            for x in (*range(X0), *range(X0 + NX, XE)):
                field[m, x] = blank
            for x in range(X0, X0 + NX):
                field[m, x, 0:Y0] = blank[0:Y0]
                field[m, x, TOP:YE] = blank[TOP:YE]
    for seam in seams:
        for m in range(2):
            for tile in (0, 3):
                seam[m, tile] = blank
            for tile in (1, 2):
                seam[m, tile, 0:Y0] = blank[0:Y0]
                seam[m, tile, TOP:YE] = blank[TOP:YE]


def build(xa, xb, z, za, zb, *refs):
    seams, (ea, eb) = refs[3:6], refs[6:]
    iz = lax.axis_index("gz")
    lane, own = lane_ids(NY), own_lanes(NY, iz)
    swap = 8 + 112 * iz

    def other(tile):
        return pltpu.roll(tile, swap, 1)

    for half in range(2):
        tiles = [z[half, n] for n in range(3)]
        halves = ((tiles[0], tiles[1]), (other(tiles[0]), other(tiles[1])), (tiles[2], other(tiles[2])))
        for f in range(3):
            for m in range(2):
                here = (m, 1 + half, slice(Y0, TOP))
                seams[f][here] = jnp.where(own, seams[f][here], halves[f][m])
    blank = jnp.zeros((NY, NZ), F32)
    for high, face, edge in zip(highs("gx"), (xa, xb), (za, zb)):
        tile = edge[...]
        for m, beyond in enumerate((tile, other(tile))):
            for f, depth, at in face_layers():
                acc = beyond if f == 0 else blank
                for layer in range(depth):
                    s = jnp.where(high == 1, layer, 8 - depth + layer)
                    turned = pltpu.roll(face[at + 2 * layer + m], (SLOT * s + 8) % NZ, 1)
                    acc = jnp.where(jnp.logical_and(lane // SLOT == s, own), turned, acc)
                seams[f][m, 3 * high, Y0:TOP] = acc
    high_x = highs("gx")
    for high, out in zip(highs("gy"), (ea, eb)):
        for row, count, side, m, away in xy_pieces():
            layer = jnp.where(high_x[side] == 1, away - 1, DX - away)
            start = high * (NY - count)
            out[row : row + count] = (xa, xb)[side][2 * layer + m, pl.ds(start, count)]
        for row, count, tile, m, f in seam_pieces():
            start = Y0 + high * (NY - count)
            out[row : row + count] = seams[f][m, tile, pl.ds(start, count)]
        out[124:128] = jnp.zeros((4, NZ), F32)


def place(xa, xb, ya, yb, *refs):
    fields = refs[3:]
    for high, face in zip(highs("gx"), (xa, xb)):
        for f, depth, at in face_layers():
            start = jnp.where(high == 1, X0 + NX, X0 - depth)
            for layer in range(depth):
                for m in range(2):
                    fields[f][m, start + layer, Y0:TOP] = face[at + 2 * layer + m]
    for high, face in zip(highs("gy"), (ya, yb)):
        for m in range(2):
            for x in range(NX):
                row = (m * NX + x) * sum(DEPTHS)
                for f, depth in enumerate(DEPTHS):
                    start = jnp.where(high == 1, TOP, Y0 - depth)
                    fields[f][m, X0 + x, pl.ds(start, depth)] = face[row : row + depth]
                    row += depth


def place_edges(ea, eb, fields, seams):
    high_x = highs("gx")
    for high, edge in zip(highs("gy"), (ea, eb)):
        for row, count, side, m, away in xy_pieces():
            x = jnp.where(high_x[side] == 1, X0 + NX - 1 + away, X0 - away)
            start = jnp.where(high == 1, TOP, Y0 - count)
            fields[0][m, x, pl.ds(start, count)] = edge[row : row + count]
        for row, count, tile, m, f in seam_pieces():
            start = jnp.where(high == 1, TOP, Y0 - count)
            seams[f][m, tile, pl.ds(start, count)] = edge[row : row + count]


def cross(a, b):
    return (
        a[1] * b[2] - a[2] * b[1],
        a[2] * b[0] - a[0] * b[2],
        a[0] * b[1] - a[1] * b[0],
    )


class Along:
    def __init__(self):
        iz = lax.axis_index("gz")
        self.iz = iz
        lane = lane_ids(8)
        self.first, self.last = lane == 0, lane == NZ - 1
        self.up_on = (1 - iz).astype(F32)
        self.down_on = iz.astype(F32)

    def slot(self, x):
        place = x - X0 + 8
        return place // 8, (119 + 2 * self.iz + NZ - SLOT * (place % 8)) % NZ

    def __call__(self, own, seam, shift):
        over = pltpu.roll(seam, shift, 1)
        up = jnp.where(self.last, over * self.up_on, pltpu.roll(own, NZ - 1, 1))
        down = jnp.where(self.first, over * self.down_on, pltpu.roll(own, 1, 1))
        return up, down


def seam_x(ref, lead, tile, rows):
    lane = lane_ids(8)
    own = ref[(*lead, tile, rows)]
    after = ref[(*lead, min(tile + 1, TILES - 1), rows)]
    before = ref[(*lead, max(tile - 1, 0), rows)]
    up = jnp.where(lane < NZ - SLOT, pltpu.roll(own, NZ - SLOT, 1), pltpu.roll(after, NZ - SLOT, 1))
    down = jnp.where(lane >= SLOT, pltpu.roll(own, SLOT, 1), pltpu.roll(before, SLOT, 1))
    return own, up, down


def chunks(rows):
    return -(-rows // 8)


def seam_gradients(C, W, T, G, Fl, depth):
    ix, iy = lax.axis_index("gx"), lax.axis_index("gy")
    lane = lane_ids(8)

    def keep(tile, y):
        place = ix * NX + (8 * tile - 8) + lane // SLOT
        row = row_ids(8) + (iy * NY - Y0) + y
        inside = jnp.logical_and(place >= 0, place < GRID_X)
        inside = jnp.logical_and(inside, jnp.logical_and(row >= 0, row < GRID_Y))
        return inside.astype(F32)

    def flux_at(k, carry):
        y = Y0 - depth - 1 + 8 * k
        here = pl.ds(y, 8)
        for tile in range(TILES):
            slope = []
            for m in range(2):
                own, after, before = seam_x(C, (m,), tile, here)
                slope.append(
                    (
                        after - before,
                        C[m, tile, pl.ds(y + 1, 8)] - C[m, tile, pl.ds(y - 1, 8)],
                        pltpu.roll(own, NZ - 1, 1) - pltpu.roll(own, 1, 1),
                    )
                )
            a, b = slope
            inside = keep(tile, y)
            crossed = tuple(inside * v for v in cross(a, b))
            for n, value in enumerate(cross(b, crossed) + cross(crossed, a)):
                Fl[n, tile, here] = value
        return carry

    lax.fori_loop(0, chunks(NY + 2 * depth + 2), flux_at, 0)

    def gradient_at(k, carry):
        y = Y0 - depth + 8 * k
        here, up, down = pl.ds(y, 8), pl.ds(y + 1, 8), pl.ds(y - 1, 8)
        for tile in range(TILES):
            inside = keep(tile, y)
            for m in range(2):
                n = 3 * m
                own, after, before = seam_x(C, (m,), tile, here)
                near = after + before + C[m, tile, up] + C[m, tile, down]
                near = near + pltpu.roll(own, NZ - 1, 1) + pltpu.roll(own, 1, 1)
                _, after, before = seam_x(Fl, (n,), tile, here)
                along = Fl[n + 2, tile, here]
                spread = after - before + (Fl[n + 1, tile, up] - Fl[n + 1, tile, down])
                spread = spread + (pltpu.roll(along, NZ - 1, 1) - pltpu.roll(along, 1, 1))
                value = W[m, tile, here] * (own - T[m, tile, here])
                value = value + (6.0 * own - near) + COUPLE * spread
                G[m, tile, here] = inside * value
        return carry

    lax.fori_loop(0, chunks(NY + 2 * depth), gradient_at, 0)


def gradients(fields, seams, G, Gs, Fl, Fs, depth):
    C, W, T = fields
    seam_gradients(*seams, Gs, Fs, depth)
    ix, iy = lax.axis_index("gx"), lax.axis_index("gy")
    along = Along()

    def keep(x, y):
        place = ix * NX + (x - X0)
        inside_x = jnp.logical_and(place >= 0, place < GRID_X).astype(F32)
        row = row_ids(8) + (iy * NY + (y - Y0))
        return jnp.where(jnp.logical_and(row >= 0, row < GRID_Y), inside_x, 0.0)

    def flux_at(x, carry):
        tile, shift = along.slot(x)
        for k in range(chunks(NY + 2 * depth + 2)):
            y = Y0 - depth - 1 + 8 * k
            here, up, down = slice(y, y + 8), slice(y + 1, y + 9), slice(y - 1, y + 7)
            slope, around = [], []
            for m in range(2):
                after, before = along(C[m, x, here], seams[0][m, tile, here], shift)
                slope.append(
                    (
                        C[m, x + 1, here] - C[m, x - 1, here],
                        C[m, x, up] - C[m, x, down],
                        after - before,
                    )
                )
                around.append(after + before)
            a, b = slope
            inside = keep(x, y)
            crossed = tuple(inside * v for v in cross(a, b))
            for m, flux in enumerate((cross(b, crossed), cross(crossed, a))):
                after, before = along(flux[2], Fs[3 * m + 2, tile, here], shift)
                Fl[3 * m, x, here] = flux[0]
                Fl[3 * m + 1, x, here] = flux[1]
                Fl[3 * m + 2, x, here] = COUPLE * (after - before) - around[m]
        return carry

    lax.fori_loop(X0 - 2, X0 + NX + 2, flux_at, 0, unroll=2)

    def gradient_at(x, carry):
        for k in range(chunks(NY + 2 * depth)):
            y = Y0 - depth + 8 * k
            here, up, down = slice(y, y + 8), slice(y + 1, y + 9), slice(y - 1, y + 7)
            inside = keep(x, y)
            for m in range(2):
                n = 3 * m
                own = C[m, x, here]
                near = (C[m, x + 1, here] + C[m, x - 1, here]) + (C[m, x, up] + C[m, x, down])
                spread = Fl[n, x + 1, here] - Fl[n, x - 1, here]
                spread = spread + (Fl[n + 1, x, up] - Fl[n + 1, x, down])
                value = W[m, x, here] * (own - T[m, x, here]) + (6.0 * own - near)
                G[m, x, here] = inside * (value + (Fl[n + 2, x, here] + COUPLE * spread))
        return carry

    lax.fori_loop(X0 - 1, X0 + NX + 1, gradient_at, 0, unroll=2)


def totals(W, G, Gs, applied, sums):
    along = Along()

    def body(x, carry):
        norm, curve = carry
        tile, shift = along.slot(x)
        for k in range(NY // 8):
            y = Y0 + 8 * k
            here, up, down = slice(y, y + 8), slice(y + 1, y + 9), slice(y - 1, y + 7)
            for m in range(2):
                own = G[m, x, here]
                after, before = along(own, Gs[m, tile, here], shift)
                near = after + G[m, x + 1, here] + G[m, x, up]
                if applied is None:
                    near = near + near
                else:
                    near = near + before + G[m, x - 1, here] + G[m, x, down]
                value = W[m, x, here] * own + (6.0 * own - near)
                if applied is not None:
                    applied[m, x - X0, 8 * k : 8 * k + 8] = value
                norm = norm + own * own
                curve = curve + own * value
        return norm, curve

    zero = jnp.zeros((8, NZ), F32)
    norm, curve = lax.fori_loop(X0, X0 + NX, body, (zero, zero))
    norm, curve = jnp.sum(norm), jnp.sum(curve)
    lane = lane_ids(8)
    row = jnp.where(lane == 0, norm, jnp.where(lane == 1, curve, 0.0))
    for k in range(sums.shape[0] // 8):
        sums[8 * k : 8 * k + 8] = row


def step_of(gathered):
    column = jnp.sum(gathered[...], axis=0, keepdims=True)
    lane = lane_ids(1)
    norm = jnp.sum(jnp.where(lane == 0, column, 0.0), axis=1, keepdims=True)
    curve = jnp.sum(jnp.where(lane == 1, column, 0.0), axis=1, keepdims=True)
    return jnp.broadcast_to(norm, (8, NZ)) / jnp.broadcast_to(curve, (8, NZ))


def sides(G, Gs, ga, gb):
    for high, out in zip(highs("gx"), (ga, gb)):
        for m in range(2):
            for layer in range(DX):
                out[2 * layer + m] = G[m, X0 + high * (NX - DX) + layer, SIDE]
            out[2 * DX + m] = Gs[m, 1 + high, SIDE]


def moved(C, Cs, G, Gs, ga, gb, step, New, News, depth):
    rows = [slice(Y0 - depth + 8 * k, Y0 - depth + 8 * k + 8) for k in range(chunks(NY + 2 * depth))]

    def body(x, carry):
        for here in rows:
            for m in range(2):
                New[m, x, here] = C[m, x, here] - step * G[m, x, here]
        return carry

    lax.fori_loop(X0, X0 + NX, body, 0)
    for tile in (1, 2):
        for here in rows:
            for m in range(2):
                News[m, tile, here] = Cs[m, tile, here] - step * Gs[m, tile, here]
    for high, side in zip(highs("gx"), (ga, gb)):
        for m in range(2):
            for k in range(SIDE_ROWS // 8):
                here, row = slice(SIDE.start + 8 * k, SIDE.start + 8 * k + 8), slice(8 * k, 8 * k + 8)
                for layer in range(DX):
                    x = high * (X0 + NX) + layer
                    New[m, x, here] = C[m, x, here] - step * side[2 * layer + m, row]
                News[m, 3 * high, here] = Cs[m, 3 * high, here] - step * side[2 * DX + m, row]


def first_step(ea, eb, *refs):
    fields, seams, (G, Gs, ga, gb, sums, Fl, Fs) = refs[6:9], refs[9:12], refs[12:]
    place_edges(ea, eb, fields, seams)
    gradients(fields, seams, G, Gs, Fl, Fs, 5)
    sides(G, Gs, ga, gb)
    totals(fields[1], G, Gs, None, sums)


def next_step(C, W, T, Cs, Ws, Ts, G, Gs, ga, gb, gathered, *refs):
    New, News, Gn, Gns, sa, sb, sums, Fl, Fs = refs
    moved(C, Cs, G, Gs, ga, gb, step_of(gathered), New, News, 5)
    gradients((New, W, T), (News, Ws, Ts), Gn, Gns, Fl, Fs, 3)
    sides(Gn, Gns, sa, sb)
    totals(W, Gn, Gns, None, sums)


def last_step(C, W, T, Cs, Ws, Ts, G, Gs, ga, gb, gathered, *refs):
    current, gradient, applied, sums, New, News, Gn, Gns, Fl, Fs = refs
    moved(C, Cs, G, Gs, ga, gb, step_of(gathered), New, News, 3)
    gradients((New, W, T), (News, Ws, Ts), Gn, Gns, Fl, Fs, 1)
    totals(W, Gn, Gns, applied, sums)

    def body(x, carry):
        for m in range(2):
            current[m, x] = New[m, X0 + x, Y0:TOP]
            gradient[m, x] = Gn[m, X0 + x, Y0:TOP]
        return carry

    lax.fori_loop(0, NX, body, 0)


def finish(current, gradient, gathered, updated):
    step = step_of(gathered)

    def body(x, carry):
        for m in range(2):
            for k in range(NY // 8):
                here = (m, x, slice(8 * k, 8 * k + 8))
                updated[here] = current[here] - step * gradient[here]
        return carry

    lax.fori_loop(0, NX, body, 0)


def call(body, outs, scratch=(), mib=2, alias=None, **more):
    return pl.pallas_call(
        body,
        out_shape=tuple(jax.ShapeDtypeStruct(s, F32) for s in outs),
        scratch_shapes=[pltpu.VMEM(s, F32) if isinstance(s, tuple) else s for s in scratch],
        compiler_params=pltpu.CompilerParams(vmem_limit_bytes=mib * 1024 * 1024),
        input_output_aliases=alias or {},
        **more,
    )


def pairs_of(size):
    first = [(i, i ^ 1) for i in range(size)]
    second = [(i, i - 1 if i % 2 == 0 else i + 1) for i in range(1, size - 1)]
    return first, second


def gather(sums):
    return lax.all_to_all(sums, ALL, 0, 0, tiled=True)


def local(models, targets, weights):
    nx, ny = lax.axis_size("gx"), lax.axis_size("gy")
    block = (2, NX, NY, NZ)
    wide, seam = (2, XE, YE, NZ), (2, TILES, YE, NZ)
    flux = ((6, XE, YE, NZ), (6, TILES, YE, NZ))
    rows = (nx * ny * 2, NZ)
    states = (wide,) * 3 + (seam,) * 3
    x_face, y_face = (2 * sum(X_DEPTHS), NY, NZ), (2 * NX * sum(DEPTHS), NZ)
    z_face, z_edge, edge = (2, 3, NY, NZ), (NY, NZ), (EDGE_ROWS, NZ)
    side = (2 * DX + 2, SIDE_ROWS, NZ)
    *state, xa, xb, ya, yb, z, za, zb = call(
        pack,
        (*states, x_face, x_face, y_face, y_face, z_face, z_edge, z_edge),
        (pltpu.SemaphoreType.DMA((6,)),),
        in_specs=[pl.BlockSpec(memory_space=pltpu.HBM)] * 3,
    )(models, weights, targets)
    first_x, second_x = pairs_of(nx)
    first_y, second_y = pairs_of(ny)

    def across(pairs):
        return [(2 * i + k, 2 * j + 1 - k) for i, j in pairs for k in range(2)]

    xa, xb = lax.ppermute(xa, "gx", first_x), lax.ppermute(xb, "gx", second_x)
    ya, yb = lax.ppermute(ya, "gy", first_y), lax.ppermute(yb, "gy", second_y)
    z = lax.ppermute(z, "gz", [(0, 1), (1, 0)])
    za = lax.ppermute(za, ("gx", "gz"), across(first_x))
    zb = lax.ppermute(zb, ("gx", "gz"), across(second_x))
    state = call(clear, states, alias={i: i for i in range(6)})(*state)
    *seams, ea, eb = call(build, (seam,) * 3 + (edge, edge), alias={5: 0, 6: 1, 7: 2})(
        xa, xb, z, za, zb, *state[3:]
    )
    ea, eb = lax.ppermute(ea, "gy", first_y), lax.ppermute(eb, "gy", second_y)
    fields = call(place, (wide,) * 3, alias={4: 0, 5: 1, 6: 2})(xa, xb, ya, yb, *state[:3])

    def refresh(ga, gb, sums):
        ga = lax.ppermute(ga, "gx", first_x)
        gb = lax.ppermute(gb, "gx", second_x)
        return ga, gb, gather(sums)

    *state, G, Gs, ga, gb, sums = call(
        first_step, (*states, wide, seam, side, side, rows), flux, 9, {2 + i: i for i in range(6)}
    )(ea, eb, *fields, *seams)
    C, Cs, G, Gs, ga, gb, sums = call(next_step, (wide, seam, wide, seam, side, side, rows), flux, 9)(
        *state, G, Gs, *refresh(ga, gb, sums)
    )
    state = (C, *state[1:3], Cs, *state[4:])
    current, gradient, applied, sums = call(
        last_step, (block, block, block, rows), (wide, seam, wide, seam, *flux), 14
    )(*state, G, Gs, *refresh(ga, gb, sums))
    (updated,) = call(finish, (block,))(current, gradient, gather(sums))
    return updated, applied


def solution(mesh):
    spec = P(None, "gx", "gy", "gz")

    return jax.shard_map(
        local, mesh=mesh, in_specs=(spec, spec, spec), out_specs=(spec, spec), check_vma=False
    )
```

```python
import jax
import jax.numpy as jnp
from jax import lax
from jax.experimental import pallas as pl
from jax.experimental.pallas import tpu as pltpu
from jax.sharding import PartitionSpec as P


ALL = ("gx", "gy", "gz")
F32 = jnp.float32
NX, NY, NZ = 16, 32, 128
DEPTHS = (7, 5, 5)
DX = 3
X_DEPTHS = (DX, 1, 1)
X0, Y0 = DX, 8
XE, YE = NX + 2 * DX, 56
TOP = Y0 + NY
GRID_X, GRID_Y = 256, 128
COUPLE = 0.05 * -2.0 * 0.0625
SLOT, TILES = 16, 4
XY_ROWS, EDGE_ROWS = 44, 128
SEAM_AT = 2 * sum(X_DEPTHS)
SIDE = slice(Y0 - 4, Y0 + NY + 4)
SIDE_ROWS = NY + 8


def lane_ids(rows):
    return lax.broadcasted_iota(jnp.int32, (rows, NZ), 1)


def row_ids(rows):
    return lax.broadcasted_iota(jnp.int32, (rows, NZ), 0)


def own_lanes(rows, iz):
    return (lane_ids(rows) % SLOT) // 8 == iz


def highs(axis):
    first = 1 - lax.axis_index(axis) % 2
    return first, 1 - first


def face_layers():
    return ((0, DX, 0), (1, 1, 2 * DX), (2, 1, 2 * DX + 2))


def xy_pieces():
    row = 0
    for side in range(2):
        for m in range(2):
            for away in (1, 2):
                yield row, 7 - away, side, m, away
                row += 7 - away


def seam_pieces():
    row = XY_ROWS
    for tile in range(TILES):
        for m in range(2):
            for f, count in ((0, 6), (1, 4), (2, 4)) if tile in (1, 2) else ((0, 6),):
                yield row, count, tile, m, f
                row += count


def pack(c, w, t, *refs):
    fields, seams, (ya, yb, z, sems) = refs[:3], refs[3:6], refs[6:]
    iz = lax.axis_index("gz")
    copies = []
    for f, source in enumerate((c, w, t)):
        for m in range(2):
            copy = pltpu.make_async_copy(
                source.at[m],
                fields[f].at[m, pl.ds(X0, NX), pl.ds(Y0, NY)],
                sems.at[2 * f + m],
            )
            copy.start()
            copies.append(copy)
    for copy in copies:
        copy.wait()
    for high, out in zip(highs("gy"), (ya, yb)):
        for m in range(2):
            for x in range(NX):
                row = (m * NX + x) * sum(DEPTHS)
                for f, depth in enumerate(DEPTHS):
                    start = Y0 + high * (NY - depth)
                    out[row : row + depth] = fields[f][m, X0 + x, pl.ds(start, depth)]
                    row += depth
    lane, own = lane_ids(NY), own_lanes(NY, iz)
    swap = 8 + 112 * iz
    for half in range(2):
        targets = []
        for m in range(2):
            packed = []
            for f in range(3):
                acc = jnp.zeros((NY, NZ), F32)
                for s in range(8):
                    block = fields[f][m, X0 + 8 * half + s, Y0:TOP]
                    turned = pltpu.roll(block, (SLOT * s + 8) % NZ, 1)
                    acc = jnp.where(jnp.logical_and(lane // SLOT == s, own), turned, acc)
                seams[f][m, 1 + half, Y0:TOP] = acc
                packed.append(acc)
            z[half, m] = packed[0] + pltpu.roll(packed[1], swap, 1)
            targets.append(packed[2])
        z[half, 2] = targets[0] + pltpu.roll(targets[1], swap, 1)


def clear(*refs):
    fields, seams = refs[6:9], refs[9:12]
    blank = jnp.zeros((YE, NZ), F32)
    for field in fields:
        for m in range(2):
            for x in (*range(X0), *range(X0 + NX, XE)):
                field[m, x] = blank
            for x in range(X0, X0 + NX):
                field[m, x, 0:Y0] = blank[0:Y0]
                field[m, x, TOP:YE] = blank[TOP:YE]
    for seam in seams:
        for m in range(2):
            for tile in (0, 3):
                seam[m, tile] = blank
            for tile in (1, 2):
                seam[m, tile, 0:Y0] = blank[0:Y0]
                seam[m, tile, TOP:YE] = blank[TOP:YE]


def merge(z, C, W, T, *refs):
    fields, seams, outs = (C, W, T), refs[3:6], refs[6:]
    iz = lax.axis_index("gz")
    own = own_lanes(NY, iz)
    swap = 8 + 112 * iz

    def other(tile):
        return pltpu.roll(tile, swap, 1)

    for half in range(2):
        tiles = [z[half, n] for n in range(3)]
        halves = ((tiles[0], tiles[1]), (other(tiles[0]), other(tiles[1])), (tiles[2], other(tiles[2])))
        for f in range(3):
            for m in range(2):
                here = (m, 1 + half, slice(Y0, TOP))
                seams[f][here] = jnp.where(own, seams[f][here], halves[f][m])
    for high, out in zip(highs("gx"), outs):
        for m in range(2):
            for f, depth, at in face_layers():
                start = X0 + high * (NX - depth)
                for layer in range(depth):
                    out[at + 2 * layer + m] = fields[f][m, start + layer, Y0:TOP]
            out[SEAM_AT + m] = seams[0][m, 1 + high, Y0:TOP]


def build(xa, xb, *refs):
    seams, (ea, eb) = refs[3:6], refs[6:]
    lane, own = lane_ids(NY), own_lanes(NY, lax.axis_index("gz"))
    for high, face in zip(highs("gx"), (xa, xb)):
        slot = jnp.where(high == 1, 0, 7)
        near = jnp.logical_and(lane // SLOT == slot, own)
        for m in range(2):
            seams[0][m, 3 * high, Y0:TOP] = face[SEAM_AT + m]
            for f, depth, at in face_layers()[1:]:
                turned = pltpu.roll(face[at + m], (SLOT * slot + 8) % NZ, 1)
                seams[f][m, 3 * high, Y0:TOP] = jnp.where(near, turned, 0.0)
    high_x = highs("gx")
    for high, out in zip(highs("gy"), (ea, eb)):
        for row, count, side, m, away in xy_pieces():
            layer = jnp.where(high_x[side] == 1, away - 1, DX - away)
            start = high * (NY - count)
            out[row : row + count] = (xa, xb)[side][2 * layer + m, pl.ds(start, count)]
        for row, count, tile, m, f in seam_pieces():
            start = Y0 + high * (NY - count)
            out[row : row + count] = seams[f][m, tile, pl.ds(start, count)]
        out[124:128] = jnp.zeros((4, NZ), F32)


def place(xa, xb, ya, yb, *refs):
    fields = refs[3:]
    for high, face in zip(highs("gx"), (xa, xb)):
        for f, depth, at in face_layers():
            start = jnp.where(high == 1, X0 + NX, X0 - depth)
            for layer in range(depth):
                for m in range(2):
                    fields[f][m, start + layer, Y0:TOP] = face[at + 2 * layer + m]
    for high, face in zip(highs("gy"), (ya, yb)):
        for m in range(2):
            for x in range(NX):
                row = (m * NX + x) * sum(DEPTHS)
                for f, depth in enumerate(DEPTHS):
                    start = jnp.where(high == 1, TOP, Y0 - depth)
                    fields[f][m, X0 + x, pl.ds(start, depth)] = face[row : row + depth]
                    row += depth


def place_edges(ea, eb, fields, seams):
    high_x = highs("gx")
    for high, edge in zip(highs("gy"), (ea, eb)):
        for row, count, side, m, away in xy_pieces():
            x = jnp.where(high_x[side] == 1, X0 + NX - 1 + away, X0 - away)
            start = jnp.where(high == 1, TOP, Y0 - count)
            fields[0][m, x, pl.ds(start, count)] = edge[row : row + count]
        for row, count, tile, m, f in seam_pieces():
            start = jnp.where(high == 1, TOP, Y0 - count)
            seams[f][m, tile, pl.ds(start, count)] = edge[row : row + count]


def cross(a, b):
    return (
        a[1] * b[2] - a[2] * b[1],
        a[2] * b[0] - a[0] * b[2],
        a[0] * b[1] - a[1] * b[0],
    )


def beside(own, first, last):
    up = jnp.where(last, 0.0, pltpu.roll(own, NZ - 1, 1))
    return up, jnp.where(first, 0.0, pltpu.roll(own, 1, 1))


class Along:
    def __init__(self):
        iz = lax.axis_index("gz")
        self.iz = iz
        lane = lane_ids(8)
        self.first, self.last = lane == 0, lane == NZ - 1
        self.up_on = (1 - iz).astype(F32)
        self.down_on = iz.astype(F32)

    def slot(self, x):
        place = x - X0 + 8
        return place // 8, (119 + 2 * self.iz + NZ - SLOT * (place % 8)) % NZ

    def __call__(self, own, seam, shift):
        over = pltpu.roll(seam, shift, 1)
        up = jnp.where(self.last, over * self.up_on, pltpu.roll(own, NZ - 1, 1))
        down = jnp.where(self.first, over * self.down_on, pltpu.roll(own, 1, 1))
        return up, down


def seam_x(ref, lead, tile, rows):
    lane = lane_ids(8)
    own = ref[(*lead, tile, rows)]
    after = ref[(*lead, min(tile + 1, TILES - 1), rows)]
    before = ref[(*lead, max(tile - 1, 0), rows)]
    up = jnp.where(lane < NZ - SLOT, pltpu.roll(own, NZ - SLOT, 1), pltpu.roll(after, NZ - SLOT, 1))
    down = jnp.where(lane >= SLOT, pltpu.roll(own, SLOT, 1), pltpu.roll(before, SLOT, 1))
    return own, up, down


def chunks(rows):
    return -(-rows // 8)


def seam_gradients(C, W, T, G, Fl, depth):
    ix, iy = lax.axis_index("gx"), lax.axis_index("gy")
    lane = lane_ids(8)

    def keep(tile, y):
        place = ix * NX + (8 * tile - 8) + lane // SLOT
        row = row_ids(8) + (iy * NY - Y0) + y
        inside = jnp.logical_and(place >= 0, place < GRID_X)
        inside = jnp.logical_and(inside, jnp.logical_and(row >= 0, row < GRID_Y))
        return inside.astype(F32)

    def flux_at(k, carry):
        y = Y0 - depth - 1 + 8 * k
        here = pl.ds(y, 8)
        for tile in range(TILES):
            slope = []
            for m in range(2):
                own, after, before = seam_x(C, (m,), tile, here)
                slope.append(
                    (
                        after - before,
                        C[m, tile, pl.ds(y + 1, 8)] - C[m, tile, pl.ds(y - 1, 8)],
                        pltpu.roll(own, NZ - 1, 1) - pltpu.roll(own, 1, 1),
                    )
                )
            a, b = slope
            inside = keep(tile, y)
            crossed = tuple(inside * v for v in cross(a, b))
            for n, value in enumerate(cross(b, crossed) + cross(crossed, a)):
                Fl[n, tile, here] = value
        return carry

    lax.fori_loop(0, chunks(NY + 2 * depth + 2), flux_at, 0)

    def gradient_at(k, carry):
        y = Y0 - depth + 8 * k
        here, up, down = pl.ds(y, 8), pl.ds(y + 1, 8), pl.ds(y - 1, 8)
        for tile in range(TILES):
            inside = keep(tile, y)
            for m in range(2):
                n = 3 * m
                own, after, before = seam_x(C, (m,), tile, here)
                near = after + before + C[m, tile, up] + C[m, tile, down]
                near = near + pltpu.roll(own, NZ - 1, 1) + pltpu.roll(own, 1, 1)
                _, after, before = seam_x(Fl, (n,), tile, here)
                along = Fl[n + 2, tile, here]
                spread = after - before + (Fl[n + 1, tile, up] - Fl[n + 1, tile, down])
                spread = spread + (pltpu.roll(along, NZ - 1, 1) - pltpu.roll(along, 1, 1))
                value = W[m, tile, here] * (own - T[m, tile, here])
                value = value + (6.0 * own - near) + COUPLE * spread
                G[m, tile, here] = inside * value
        return carry

    lax.fori_loop(0, chunks(NY + 2 * depth), gradient_at, 0)


def gradients(fields, seams, G, Gs, Fl, Fs, depth):
    C, W, T = fields
    seam_gradients(*seams, Gs, Fs, depth)
    ix, iy, iz = (lax.axis_index(axis) for axis in ALL)
    lane = lane_ids(8)
    first, last = lane == 0, lane == NZ - 1
    cut = lane - (NZ - 2) * (1 - iz)
    cut = jnp.logical_and(cut >= 0, cut < 2)

    def keep(x, y):
        place = ix * NX + (x - X0)
        inside_x = jnp.logical_and(place >= 0, place < GRID_X).astype(F32)
        row = row_ids(8) + (iy * NY + (y - Y0))
        return jnp.where(jnp.logical_and(row >= 0, row < GRID_Y), inside_x, 0.0)

    def flux_at(x, carry):
        for k in range(chunks(NY + 2 * depth + 2)):
            y = Y0 - depth - 1 + 8 * k
            here, up, down = slice(y, y + 8), slice(y + 1, y + 9), slice(y - 1, y + 7)
            slope, around = [], []
            for m in range(2):
                after, before = beside(C[m, x, here], first, last)
                slope.append(
                    (
                        C[m, x + 1, here] - C[m, x - 1, here],
                        C[m, x, up] - C[m, x, down],
                        after - before,
                    )
                )
                around.append(after + before)
            a, b = slope
            inside = keep(x, y)
            crossed = tuple(inside * v for v in cross(a, b))
            for m, flux in enumerate((cross(b, crossed), cross(crossed, a))):
                after, before = beside(flux[2], first, last)
                Fl[3 * m, x, here] = flux[0]
                Fl[3 * m + 1, x, here] = flux[1]
                Fl[3 * m + 2, x, here] = COUPLE * (after - before) - around[m]
        return carry

    lax.fori_loop(X0 - 2, X0 + NX + 2, flux_at, 0, unroll=2)

    def gradient_at(x, carry):
        place = x - X0 + 8
        tile, shift = place // 8, (120 + NZ - SLOT * (place % 8)) % NZ
        for k in range(chunks(NY + 2 * depth)):
            y = Y0 - depth + 8 * k
            here, up, down = slice(y, y + 8), slice(y + 1, y + 9), slice(y - 1, y + 7)
            inside = keep(x, y)
            for m in range(2):
                n = 3 * m
                own = C[m, x, here]
                near = (C[m, x + 1, here] + C[m, x - 1, here]) + (C[m, x, up] + C[m, x, down])
                spread = Fl[n, x + 1, here] - Fl[n, x - 1, here]
                spread = spread + (Fl[n + 1, x, up] - Fl[n + 1, x, down])
                value = W[m, x, here] * (own - T[m, x, here]) + (6.0 * own - near)
                value = inside * (value + (Fl[n + 2, x, here] + COUPLE * spread))
                G[m, x, here] = jnp.where(cut, pltpu.roll(Gs[m, tile, here], shift, 1), value)
        return carry

    lax.fori_loop(X0 - 1, X0 + NX + 1, gradient_at, 0, unroll=2)


def totals(W, G, Gs, applied, sums):
    along = Along()

    def body(x, carry):
        norm, curve = carry
        tile, shift = along.slot(x)
        for k in range(NY // 8):
            y = Y0 + 8 * k
            here, up, down = slice(y, y + 8), slice(y + 1, y + 9), slice(y - 1, y + 7)
            for m in range(2):
                own = G[m, x, here]
                after, before = along(own, Gs[m, tile, here], shift)
                near = after + G[m, x + 1, here] + G[m, x, up]
                if applied is None:
                    near = near + near
                else:
                    near = near + before + G[m, x - 1, here] + G[m, x, down]
                value = W[m, x, here] * own + (6.0 * own - near)
                if applied is not None:
                    applied[m, x - X0, 8 * k : 8 * k + 8] = value
                norm = norm + own * own
                curve = curve + own * value
        return norm, curve

    zero = jnp.zeros((8, NZ), F32)
    norm, curve = lax.fori_loop(X0, X0 + NX, body, (zero, zero))
    norm, curve = (jnp.sum(v, axis=0, keepdims=True) for v in (norm, curve))
    row = jnp.where(lane_ids(1) < NZ // 2, norm + pltpu.roll(norm, 64, 1), curve + pltpu.roll(curve, 64, 1))
    row = jnp.broadcast_to(row, (8, NZ))
    for k in range(sums.shape[0] // 8):
        sums[8 * k : 8 * k + 8] = row


def step_of(gathered):
    column = jnp.sum(gathered[...], axis=0, keepdims=True)
    lane = lane_ids(1)
    norm = jnp.sum(jnp.where(lane < NZ // 2, column, 0.0), axis=1, keepdims=True)
    curve = jnp.sum(jnp.where(lane >= NZ // 2, column, 0.0), axis=1, keepdims=True)
    return jnp.broadcast_to(norm, (8, NZ)) / jnp.broadcast_to(curve, (8, NZ))


def sides(G, Gs, ga, gb):
    for high, out in zip(highs("gx"), (ga, gb)):
        for m in range(2):
            for layer in range(DX):
                out[2 * layer + m] = G[m, X0 + high * (NX - DX) + layer, SIDE]
            out[2 * DX + m] = Gs[m, 1 + high, SIDE]


def moved(C, Cs, G, Gs, ga, gb, step, New, News, depth):
    rows = [slice(Y0 - depth + 8 * k, Y0 - depth + 8 * k + 8) for k in range(chunks(NY + 2 * depth))]

    def body(x, carry):
        for here in rows:
            for m in range(2):
                New[m, x, here] = C[m, x, here] - step * G[m, x, here]
        return carry

    lax.fori_loop(X0, X0 + NX, body, 0)
    for tile in (1, 2):
        for here in rows:
            for m in range(2):
                News[m, tile, here] = Cs[m, tile, here] - step * Gs[m, tile, here]
    for high, side in zip(highs("gx"), (ga, gb)):
        for m in range(2):
            for k in range(SIDE_ROWS // 8):
                here, row = slice(SIDE.start + 8 * k, SIDE.start + 8 * k + 8), slice(8 * k, 8 * k + 8)
                for layer in range(DX):
                    x = high * (X0 + NX) + layer
                    New[m, x, here] = C[m, x, here] - step * side[2 * layer + m, row]
                News[m, 3 * high, here] = Cs[m, 3 * high, here] - step * side[2 * DX + m, row]


def first_step(ea, eb, *refs):
    fields, seams, (G, Gs, ga, gb, sums, Fl, Fs) = refs[6:9], refs[9:12], refs[12:]
    place_edges(ea, eb, fields, seams)
    gradients(fields, seams, G, Gs, Fl, Fs, 5)
    sides(G, Gs, ga, gb)
    totals(fields[1], G, Gs, None, sums)


def next_step(C, W, T, Cs, Ws, Ts, G, Gs, ga, gb, gathered, *refs):
    New, News, Gn, Gns, sa, sb, sums, Fl, Fs = refs
    moved(C, Cs, G, Gs, ga, gb, step_of(gathered), New, News, 5)
    gradients((New, W, T), (News, Ws, Ts), Gn, Gns, Fl, Fs, 3)
    sides(Gn, Gns, sa, sb)
    totals(W, Gn, Gns, None, sums)


def last_step(C, W, T, Cs, Ws, Ts, G, Gs, ga, gb, gathered, *refs):
    current, gradient, applied, sums, New, News, Gn, Gns, Fl, Fs = refs
    moved(C, Cs, G, Gs, ga, gb, step_of(gathered), New, News, 3)
    gradients((New, W, T), (News, Ws, Ts), Gn, Gns, Fl, Fs, 1)
    totals(W, Gn, Gns, applied, sums)

    def body(x, carry):
        for m in range(2):
            current[m, x] = New[m, X0 + x, Y0:TOP]
            gradient[m, x] = Gn[m, X0 + x, Y0:TOP]
        return carry

    lax.fori_loop(0, NX, body, 0)


def finish(current, gradient, gathered, updated):
    step = step_of(gathered)

    def body(x, carry):
        for m in range(2):
            for k in range(NY // 8):
                here = (m, x, slice(8 * k, 8 * k + 8))
                updated[here] = current[here] - step * gradient[here]
        return carry

    lax.fori_loop(0, NX, body, 0)


def call(body, outs, scratch=(), mib=2, alias=None, **more):
    return pl.pallas_call(
        body,
        out_shape=tuple(jax.ShapeDtypeStruct(s, F32) for s in outs),
        scratch_shapes=[pltpu.VMEM(s, F32) if isinstance(s, tuple) else s for s in scratch],
        compiler_params=pltpu.CompilerParams(vmem_limit_bytes=mib * 1024 * 1024),
        input_output_aliases=alias or {},
        **more,
    )


def pairs_of(size):
    first = [(i, i ^ 1) for i in range(size)]
    second = [(i, i - 1 if i % 2 == 0 else i + 1) for i in range(1, size - 1)]
    return first, second


def gather(sums):
    return lax.all_to_all(sums, ALL, 0, 0, tiled=True)


def local(models, targets, weights):
    nx, ny = lax.axis_size("gx"), lax.axis_size("gy")
    block = (2, NX, NY, NZ)
    wide, seam = (2, XE, YE, NZ), (2, TILES, YE, NZ)
    flux = ((6, XE, YE, NZ), (6, TILES, YE, NZ))
    rows = (nx * ny * 2, NZ)
    states = (wide,) * 3 + (seam,) * 3
    x_face, y_face = (SEAM_AT + 2, NY, NZ), (2 * NX * sum(DEPTHS), NZ)
    edge, side = (EDGE_ROWS, NZ), (2 * DX + 2, SIDE_ROWS, NZ)
    *state, ya, yb, z = call(
        pack,
        (*states, y_face, y_face, (2, 3, NY, NZ)),
        (pltpu.SemaphoreType.DMA((6,)),),
        in_specs=[pl.BlockSpec(memory_space=pltpu.HBM)] * 3,
    )(models, weights, targets)
    first_x, second_x = pairs_of(nx)
    first_y, second_y = pairs_of(ny)
    z = lax.ppermute(z, "gz", [(0, 1), (1, 0)])
    ya = lax.ppermute(ya, "gy", first_y)
    *seams, xa, xb = call(merge, (seam,) * 3 + (x_face, x_face), alias={4: 0, 5: 1, 6: 2})(z, *state)
    xa, xb = lax.ppermute(xa, "gx", first_x), lax.ppermute(xb, "gx", second_x)
    yb = lax.ppermute(yb, "gy", second_y)
    state = call(clear, states, alias={i: i for i in range(6)})(*state[:3], *seams)
    *seams, ea, eb = call(build, (seam,) * 3 + (edge, edge), alias={2: 0, 3: 1, 4: 2})(
        xa, xb, *state[3:]
    )
    ea, eb = lax.ppermute(ea, "gy", first_y), lax.ppermute(eb, "gy", second_y)
    fields = call(place, (wide,) * 3, alias={4: 0, 5: 1, 6: 2})(xa, xb, ya, yb, *state[:3])

    def refresh(ga, gb, sums):
        ga = lax.ppermute(ga, "gx", first_x)
        gb = lax.ppermute(gb, "gx", second_x)
        return ga, gb, gather(sums)

    *state, G, Gs, ga, gb, sums = call(
        first_step, (*states, wide, seam, side, side, rows), flux, 9, {2 + i: i for i in range(6)}
    )(ea, eb, *fields, *seams)
    C, Cs, G, Gs, ga, gb, sums = call(next_step, (wide, seam, wide, seam, side, side, rows), flux, 9)(
        *state, G, Gs, *refresh(ga, gb, sums)
    )
    state = (C, *state[1:3], Cs, *state[4:])
    current, gradient, applied, sums = call(
        last_step, (block, block, block, rows), (wide, seam, wide, seam, *flux), 14
    )(*state, G, Gs, *refresh(ga, gb, sums))
    (updated,) = call(finish, (block,))(current, gradient, gather(sums))
    return updated, applied


def solution(mesh):
    spec = P(None, "gx", "gy", "gz")

    return jax.shard_map(
        local, mesh=mesh, in_specs=(spec, spec, spec), out_specs=(spec, spec), check_vma=False
    )
```

```python
import jax
import jax.numpy as jnp
from jax import lax
from jax.experimental import pallas as pl
from jax.experimental.pallas import tpu as pltpu
from jax.sharding import PartitionSpec as P


ALL = ("gx", "gy", "gz")
F32 = jnp.float32
NX, NY, NZ = 16, 32, 128
DEPTHS = (7, 5, 5)
DX = 3
X_DEPTHS = (DX, 1, 1)
X0, Y0 = DX, 8
XE, YE = NX + 2 * DX, 56
TOP = Y0 + NY
GRID_X, GRID_Y = 256, 128
COUPLE = 0.05 * -2.0 * 0.0625
SLOT, TILES = 16, 4
XY_ROWS, EDGE_ROWS = 44, 128
SEAM_AT = 2 * sum(X_DEPTHS)
SIDE = slice(Y0 - 4, Y0 + NY + 4)
SIDE_ROWS = NY + 8
UNROLL, SEAM_UNROLL = 2, 1


def lane_ids(rows):
    return lax.broadcasted_iota(jnp.int32, (rows, NZ), 1)


def row_ids(rows):
    return lax.broadcasted_iota(jnp.int32, (rows, NZ), 0)


def own_lanes(rows, iz):
    return (lane_ids(rows) % SLOT) // 8 == iz


def highs(axis):
    first = 1 - lax.axis_index(axis) % 2
    return first, 1 - first


def face_layers():
    return ((0, DX, 0), (1, 1, 2 * DX), (2, 1, 2 * DX + 2))


def xy_pieces():
    row = 0
    for side in range(2):
        for m in range(2):
            for away in (1, 2):
                yield row, 7 - away, side, m, away
                row += 7 - away


def seam_pieces():
    row = XY_ROWS
    for tile in range(TILES):
        for m in range(2):
            for f, count in ((0, 6), (1, 4), (2, 4)) if tile in (1, 2) else ((0, 6),):
                yield row, count, tile, m, f
                row += count


def pack(c, w, t, *refs):
    fields, seams, (ya, yb, z, sems) = refs[:3], refs[3:6], refs[6:]
    iz = lax.axis_index("gz")
    copies = []
    for f, source in enumerate((c, w, t)):
        for m in range(2):
            copy = pltpu.make_async_copy(
                source.at[m],
                fields[f].at[m, pl.ds(X0, NX), pl.ds(Y0, NY)],
                sems.at[2 * f + m],
            )
            copy.start()
            copies.append(copy)
    for copy in copies:
        copy.wait()
    for high, out in zip(highs("gy"), (ya, yb)):
        for m in range(2):
            for x in range(NX):
                row = (m * NX + x) * sum(DEPTHS)
                for f, depth in enumerate(DEPTHS):
                    start = Y0 + high * (NY - depth)
                    out[row : row + depth] = fields[f][m, X0 + x, pl.ds(start, depth)]
                    row += depth
    lane, own = lane_ids(NY), own_lanes(NY, iz)
    swap = 8 + 112 * iz
    for half in range(2):
        targets = []
        for m in range(2):
            packed = []
            for f in range(3):
                acc = jnp.zeros((NY, NZ), F32)
                for s in range(8):
                    block = fields[f][m, X0 + 8 * half + s, Y0:TOP]
                    turned = pltpu.roll(block, (SLOT * s + 8) % NZ, 1)
                    acc = jnp.where(jnp.logical_and(lane // SLOT == s, own), turned, acc)
                seams[f][m, 1 + half, Y0:TOP] = acc
                packed.append(acc)
            z[half, m] = packed[0] + pltpu.roll(packed[1], swap, 1)
            targets.append(packed[2])
        z[half, 2] = targets[0] + pltpu.roll(targets[1], swap, 1)


def clear(*refs):
    fields, seams = refs[6:9], refs[9:12]
    blank = jnp.zeros((YE, NZ), F32)
    for field in fields:
        for m in range(2):
            for x in (*range(X0), *range(X0 + NX, XE)):
                field[m, x] = blank
            for x in range(X0, X0 + NX):
                field[m, x, 0:Y0] = blank[0:Y0]
                field[m, x, TOP:YE] = blank[TOP:YE]
    for seam in seams:
        for m in range(2):
            for tile in (0, 3):
                seam[m, tile] = blank
            for tile in (1, 2):
                seam[m, tile, 0:Y0] = blank[0:Y0]
                seam[m, tile, TOP:YE] = blank[TOP:YE]


def merge(z, C, W, T, *refs):
    fields, seams, outs = (C, W, T), refs[3:6], refs[6:]
    iz = lax.axis_index("gz")
    own = own_lanes(NY, iz)
    swap = 8 + 112 * iz

    def other(tile):
        return pltpu.roll(tile, swap, 1)

    for half in range(2):
        tiles = [z[half, n] for n in range(3)]
        halves = ((tiles[0], tiles[1]), (other(tiles[0]), other(tiles[1])), (tiles[2], other(tiles[2])))
        for f in range(3):
            for m in range(2):
                here = (m, 1 + half, slice(Y0, TOP))
                seams[f][here] = jnp.where(own, seams[f][here], halves[f][m])
    for high, out in zip(highs("gx"), outs):
        for m in range(2):
            for f, depth, at in face_layers():
                start = X0 + high * (NX - depth)
                for layer in range(depth):
                    out[at + 2 * layer + m] = fields[f][m, start + layer, Y0:TOP]
            out[SEAM_AT + m] = seams[0][m, 1 + high, Y0:TOP]


def build(xa, xb, *refs):
    seams, (ea, eb) = refs[3:6], refs[6:]
    lane, own = lane_ids(NY), own_lanes(NY, lax.axis_index("gz"))
    for high, face in zip(highs("gx"), (xa, xb)):
        slot = jnp.where(high == 1, 0, 7)
        near = jnp.logical_and(lane // SLOT == slot, own)
        for m in range(2):
            seams[0][m, 3 * high, Y0:TOP] = face[SEAM_AT + m]
            for f, depth, at in face_layers()[1:]:
                turned = pltpu.roll(face[at + m], (SLOT * slot + 8) % NZ, 1)
                seams[f][m, 3 * high, Y0:TOP] = jnp.where(near, turned, 0.0)
    high_x = highs("gx")
    for high, out in zip(highs("gy"), (ea, eb)):
        for row, count, side, m, away in xy_pieces():
            layer = jnp.where(high_x[side] == 1, away - 1, DX - away)
            start = high * (NY - count)
            out[row : row + count] = (xa, xb)[side][2 * layer + m, pl.ds(start, count)]
        for row, count, tile, m, f in seam_pieces():
            start = Y0 + high * (NY - count)
            out[row : row + count] = seams[f][m, tile, pl.ds(start, count)]
        out[124:128] = jnp.zeros((4, NZ), F32)


def place(xa, xb, ya, yb, *refs):
    fields = refs[3:]
    for high, face in zip(highs("gx"), (xa, xb)):
        for f, depth, at in face_layers():
            start = jnp.where(high == 1, X0 + NX, X0 - depth)
            for layer in range(depth):
                for m in range(2):
                    fields[f][m, start + layer, Y0:TOP] = face[at + 2 * layer + m]
    for high, face in zip(highs("gy"), (ya, yb)):
        for m in range(2):
            for x in range(NX):
                row = (m * NX + x) * sum(DEPTHS)
                for f, depth in enumerate(DEPTHS):
                    start = jnp.where(high == 1, TOP, Y0 - depth)
                    fields[f][m, X0 + x, pl.ds(start, depth)] = face[row : row + depth]
                    row += depth


def place_edges(ea, eb, fields, seams):
    high_x = highs("gx")
    for high, edge in zip(highs("gy"), (ea, eb)):
        for row, count, side, m, away in xy_pieces():
            x = jnp.where(high_x[side] == 1, X0 + NX - 1 + away, X0 - away)
            start = jnp.where(high == 1, TOP, Y0 - count)
            fields[0][m, x, pl.ds(start, count)] = edge[row : row + count]
        for row, count, tile, m, f in seam_pieces():
            start = jnp.where(high == 1, TOP, Y0 - count)
            seams[f][m, tile, pl.ds(start, count)] = edge[row : row + count]


def cross(a, b):
    return (
        a[1] * b[2] - a[2] * b[1],
        a[2] * b[0] - a[0] * b[2],
        a[0] * b[1] - a[1] * b[0],
    )


def beside(own, first, last):
    up = jnp.where(last, 0.0, pltpu.roll(own, NZ - 1, 1))
    return up, jnp.where(first, 0.0, pltpu.roll(own, 1, 1))


class Along:
    def __init__(self):
        iz = lax.axis_index("gz")
        self.iz = iz
        lane = lane_ids(8)
        self.first, self.last = lane == 0, lane == NZ - 1
        self.up_on = (1 - iz).astype(F32)
        self.down_on = iz.astype(F32)

    def slot(self, x):
        place = x - X0 + 8
        return place // 8, (119 + 2 * self.iz + NZ - SLOT * (place % 8)) % NZ

    def __call__(self, own, seam, shift):
        over = pltpu.roll(seam, shift, 1)
        up = jnp.where(self.last, over * self.up_on, pltpu.roll(own, NZ - 1, 1))
        down = jnp.where(self.first, over * self.down_on, pltpu.roll(own, 1, 1))
        return up, down


def seam_x(ref, lead, tile, rows):
    lane = lane_ids(8)
    own = ref[(*lead, tile, rows)]
    after = ref[(*lead, min(tile + 1, TILES - 1), rows)]
    before = ref[(*lead, max(tile - 1, 0), rows)]
    up = jnp.where(lane < NZ - SLOT, pltpu.roll(own, NZ - SLOT, 1), pltpu.roll(after, NZ - SLOT, 1))
    down = jnp.where(lane >= SLOT, pltpu.roll(own, SLOT, 1), pltpu.roll(before, SLOT, 1))
    return own, up, down


def chunks(rows):
    return -(-rows // 8)


def seam_gradients(C, W, T, G, Fl, depth):
    ix, iy = lax.axis_index("gx"), lax.axis_index("gy")
    lane = lane_ids(8)

    def keep(tile, y):
        place = ix * NX + (8 * tile - 8) + lane // SLOT
        row = row_ids(8) + (iy * NY - Y0) + y
        inside = jnp.logical_and(place >= 0, place < GRID_X)
        inside = jnp.logical_and(inside, jnp.logical_and(row >= 0, row < GRID_Y))
        return inside.astype(F32)

    def flux_at(k, carry):
        y = Y0 - depth - 1 + 8 * k
        here = pl.ds(y, 8)
        for tile in range(TILES):
            slope = []
            for m in range(2):
                own, after, before = seam_x(C, (m,), tile, here)
                slope.append(
                    (
                        after - before,
                        C[m, tile, pl.ds(y + 1, 8)] - C[m, tile, pl.ds(y - 1, 8)],
                        pltpu.roll(own, NZ - 1, 1) - pltpu.roll(own, 1, 1),
                    )
                )
            a, b = slope
            inside = keep(tile, y)
            crossed = tuple(inside * v for v in cross(a, b))
            for n, value in enumerate(cross(b, crossed) + cross(crossed, a)):
                Fl[n, tile, here] = value
        return carry

    lax.fori_loop(0, chunks(NY + 2 * depth + 2), flux_at, 0, unroll=SEAM_UNROLL)

    def gradient_at(k, carry):
        y = Y0 - depth + 8 * k
        here, up, down = pl.ds(y, 8), pl.ds(y + 1, 8), pl.ds(y - 1, 8)
        for tile in range(TILES):
            inside = keep(tile, y)
            for m in range(2):
                n = 3 * m
                own, after, before = seam_x(C, (m,), tile, here)
                near = after + before + C[m, tile, up] + C[m, tile, down]
                near = near + pltpu.roll(own, NZ - 1, 1) + pltpu.roll(own, 1, 1)
                _, after, before = seam_x(Fl, (n,), tile, here)
                along = Fl[n + 2, tile, here]
                spread = after - before + (Fl[n + 1, tile, up] - Fl[n + 1, tile, down])
                spread = spread + (pltpu.roll(along, NZ - 1, 1) - pltpu.roll(along, 1, 1))
                value = W[m, tile, here] * (own - T[m, tile, here])
                value = value + (6.0 * own - near) + COUPLE * spread
                G[m, tile, here] = inside * value
        return carry

    lax.fori_loop(0, chunks(NY + 2 * depth), gradient_at, 0, unroll=SEAM_UNROLL)


def gradients(fields, seams, G, Gs, Fl, Fs, depth):
    C, W, T = fields
    seam_gradients(*seams, Gs, Fs, depth)
    ix, iy, iz = (lax.axis_index(axis) for axis in ALL)
    lane = lane_ids(8)
    first, last = lane == 0, lane == NZ - 1
    cut = lane - (NZ - 2) * (1 - iz)
    cut = jnp.logical_and(cut >= 0, cut < 2)

    def keep(x, y):
        place = ix * NX + (x - X0)
        inside_x = jnp.logical_and(place >= 0, place < GRID_X).astype(F32)
        row = row_ids(8) + (iy * NY + (y - Y0))
        return jnp.where(jnp.logical_and(row >= 0, row < GRID_Y), inside_x, 0.0)

    def flux_at(x, carry):
        for k in range(chunks(NY + 2 * depth + 2)):
            y = Y0 - depth - 1 + 8 * k
            here, up, down = slice(y, y + 8), slice(y + 1, y + 9), slice(y - 1, y + 7)
            slope, around = [], []
            for m in range(2):
                after, before = beside(C[m, x, here], first, last)
                slope.append(
                    (
                        C[m, x + 1, here] - C[m, x - 1, here],
                        C[m, x, up] - C[m, x, down],
                        after - before,
                    )
                )
                around.append(after + before)
            a, b = slope
            inside = keep(x, y)
            crossed = tuple(inside * v for v in cross(a, b))
            for m, flux in enumerate((cross(b, crossed), cross(crossed, a))):
                after, before = beside(flux[2], first, last)
                Fl[3 * m, x, here] = flux[0]
                Fl[3 * m + 1, x, here] = flux[1]
                Fl[3 * m + 2, x, here] = COUPLE * (after - before) - around[m]
        return carry

    def gradient_at(x, carry):
        place = x - X0 + 8
        tile, shift = place // 8, (120 + NZ - SLOT * (place % 8)) % NZ
        for k in range(chunks(NY + 2 * depth)):
            y = Y0 - depth + 8 * k
            here, up, down = slice(y, y + 8), slice(y + 1, y + 9), slice(y - 1, y + 7)
            inside = keep(x, y)
            for m in range(2):
                n = 3 * m
                own = C[m, x, here]
                near = (C[m, x + 1, here] + C[m, x - 1, here]) + (C[m, x, up] + C[m, x, down])
                spread = Fl[n, x + 1, here] - Fl[n, x - 1, here]
                spread = spread + (Fl[n + 1, x, up] - Fl[n + 1, x, down])
                value = W[m, x, here] * (own - T[m, x, here]) + (6.0 * own - near)
                value = inside * (value + (Fl[n + 2, x, here] + COUPLE * spread))
                G[m, x, here] = jnp.where(cut, pltpu.roll(Gs[m, tile, here], shift, 1), value)
        return carry

    def pair_at(x, fluxes, slopes):
        if fluxes:
            flux_at(x, 0)
            flux_at(x + 1, 0)
        if slopes:
            gradient_at(x - 3, 0)
            gradient_at(x - 2, 0)

    def both_at(i, carry):
        pair_at(X0 - 2 + 2 * i, True, True)
        return carry

    def lead_at(i, carry):
        pair_at(X0 - 2 + 2 * i, True, False)
        return carry

    lax.fori_loop(0, 2, lead_at, 0)
    lax.fori_loop(2, NX // 2 + 2, both_at, 0)
    pair_at(X0 + NX + 2, False, True)


def totals(W, G, Gs, applied, sums):
    along = Along()

    def body(x, carry):
        norm, curve = carry
        tile, shift = along.slot(x)
        for k in range(NY // 8):
            y = Y0 + 8 * k
            here, up, down = slice(y, y + 8), slice(y + 1, y + 9), slice(y - 1, y + 7)
            for m in range(2):
                own = G[m, x, here]
                after, before = along(own, Gs[m, tile, here], shift)
                near = after + G[m, x + 1, here] + G[m, x, up]
                if applied is None:
                    near = near + near
                else:
                    near = near + before + G[m, x - 1, here] + G[m, x, down]
                value = W[m, x, here] * own + (6.0 * own - near)
                if applied is not None:
                    applied[m, x - X0, 8 * k : 8 * k + 8] = value
                norm = norm + own * own
                curve = curve + own * value
        return norm, curve

    zero = jnp.zeros((8, NZ), F32)
    norm, curve = lax.fori_loop(X0, X0 + NX, body, (zero, zero), unroll=UNROLL)
    norm, curve = (jnp.sum(v, axis=0, keepdims=True) for v in (norm, curve))
    row = jnp.where(lane_ids(1) < NZ // 2, norm + pltpu.roll(norm, 64, 1), curve + pltpu.roll(curve, 64, 1))
    row = jnp.broadcast_to(row, (8, NZ))
    for k in range(sums.shape[0] // 8):
        sums[8 * k : 8 * k + 8] = row


def step_of(gathered):
    column = jnp.sum(gathered[...], axis=0, keepdims=True)
    lane = lane_ids(1)
    norm = jnp.sum(jnp.where(lane < NZ // 2, column, 0.0), axis=1, keepdims=True)
    curve = jnp.sum(jnp.where(lane >= NZ // 2, column, 0.0), axis=1, keepdims=True)
    return jnp.broadcast_to(norm, (8, NZ)) / jnp.broadcast_to(curve, (8, NZ))


def sides(G, Gs, ga, gb):
    for high, out in zip(highs("gx"), (ga, gb)):
        for m in range(2):
            for layer in range(DX):
                out[2 * layer + m] = G[m, X0 + high * (NX - DX) + layer, SIDE]
            out[2 * DX + m] = Gs[m, 1 + high, SIDE]


def moved(C, Cs, G, Gs, ga, gb, step, New, News, depth):
    rows = [slice(Y0 - depth + 8 * k, Y0 - depth + 8 * k + 8) for k in range(chunks(NY + 2 * depth))]

    def body(x, carry):
        for here in rows:
            for m in range(2):
                New[m, x, here] = C[m, x, here] - step * G[m, x, here]
        return carry

    lax.fori_loop(X0, X0 + NX, body, 0)
    for tile in (1, 2):
        for here in rows:
            for m in range(2):
                News[m, tile, here] = Cs[m, tile, here] - step * Gs[m, tile, here]
    for high, side in zip(highs("gx"), (ga, gb)):
        for m in range(2):
            for k in range(SIDE_ROWS // 8):
                here, row = slice(SIDE.start + 8 * k, SIDE.start + 8 * k + 8), slice(8 * k, 8 * k + 8)
                for layer in range(DX):
                    x = high * (X0 + NX) + layer
                    New[m, x, here] = C[m, x, here] - step * side[2 * layer + m, row]
                News[m, 3 * high, here] = Cs[m, 3 * high, here] - step * side[2 * DX + m, row]


def first_step(ea, eb, *refs):
    fields, seams, (G, Gs, ga, gb, sums, Fl, Fs) = refs[6:9], refs[9:12], refs[12:]
    place_edges(ea, eb, fields, seams)
    gradients(fields, seams, G, Gs, Fl, Fs, 5)
    sides(G, Gs, ga, gb)
    totals(fields[1], G, Gs, None, sums)


def next_step(C, W, T, Cs, Ws, Ts, G, Gs, ga, gb, gathered, *refs):
    New, News, Gn, Gns, sa, sb, sums, Fl, Fs = refs
    moved(C, Cs, G, Gs, ga, gb, step_of(gathered), New, News, 5)
    gradients((New, W, T), (News, Ws, Ts), Gn, Gns, Fl, Fs, 3)
    sides(Gn, Gns, sa, sb)
    totals(W, Gn, Gns, None, sums)


def last_step(C, W, T, Cs, Ws, Ts, G, Gs, ga, gb, gathered, *refs):
    current, gradient, applied, sums, New, News, Gn, Gns, Fl, Fs = refs
    moved(C, Cs, G, Gs, ga, gb, step_of(gathered), New, News, 3)
    gradients((New, W, T), (News, Ws, Ts), Gn, Gns, Fl, Fs, 1)
    totals(W, Gn, Gns, applied, sums)

    def body(x, carry):
        for m in range(2):
            current[m, x] = New[m, X0 + x, Y0:TOP]
            gradient[m, x] = Gn[m, X0 + x, Y0:TOP]
        return carry

    lax.fori_loop(0, NX, body, 0)


def finish(current, gradient, gathered, updated):
    step = step_of(gathered)

    def body(x, carry):
        for m in range(2):
            for k in range(NY // 8):
                here = (m, x, slice(8 * k, 8 * k + 8))
                updated[here] = current[here] - step * gradient[here]
        return carry

    lax.fori_loop(0, NX, body, 0)


def call(body, outs, scratch=(), mib=2, alias=None, **more):
    return pl.pallas_call(
        body,
        out_shape=tuple(jax.ShapeDtypeStruct(s, F32) for s in outs),
        scratch_shapes=[pltpu.VMEM(s, F32) if isinstance(s, tuple) else s for s in scratch],
        compiler_params=pltpu.CompilerParams(vmem_limit_bytes=mib * 1024 * 1024),
        input_output_aliases=alias or {},
        **more,
    )


def pairs_of(size):
    first = [(i, i ^ 1) for i in range(size)]
    second = [(i, i - 1 if i % 2 == 0 else i + 1) for i in range(1, size - 1)]
    return first, second


def gather(sums):
    return lax.all_to_all(sums, ALL, 0, 0, tiled=True)


def local(models, targets, weights):
    nx, ny = lax.axis_size("gx"), lax.axis_size("gy")
    block = (2, NX, NY, NZ)
    wide, seam = (2, XE, YE, NZ), (2, TILES, YE, NZ)
    flux = ((6, XE, YE, NZ), (6, TILES, YE, NZ))
    rows = (nx * ny * 2, NZ)
    states = (wide,) * 3 + (seam,) * 3
    x_face, y_face = (SEAM_AT + 2, NY, NZ), (2 * NX * sum(DEPTHS), NZ)
    edge, side = (EDGE_ROWS, NZ), (2 * DX + 2, SIDE_ROWS, NZ)
    *state, ya, yb, z = call(
        pack,
        (*states, y_face, y_face, (2, 3, NY, NZ)),
        (pltpu.SemaphoreType.DMA((6,)),),
        in_specs=[pl.BlockSpec(memory_space=pltpu.HBM)] * 3,
    )(models, weights, targets)
    first_x, second_x = pairs_of(nx)
    first_y, second_y = pairs_of(ny)
    z = lax.ppermute(z, "gz", [(0, 1), (1, 0)])
    ya = lax.ppermute(ya, "gy", first_y)
    *seams, xa, xb = call(merge, (seam,) * 3 + (x_face, x_face), alias={4: 0, 5: 1, 6: 2})(z, *state)
    xa, xb = lax.ppermute(xa, "gx", first_x), lax.ppermute(xb, "gx", second_x)
    yb = lax.ppermute(yb, "gy", second_y)
    state = call(clear, states, alias={i: i for i in range(6)})(*state[:3], *seams)
    *seams, ea, eb = call(build, (seam,) * 3 + (edge, edge), alias={2: 0, 3: 1, 4: 2})(
        xa, xb, *state[3:]
    )
    ea, eb = lax.ppermute(ea, "gy", first_y), lax.ppermute(eb, "gy", second_y)
    fields = call(place, (wide,) * 3, alias={4: 0, 5: 1, 6: 2})(xa, xb, ya, yb, *state[:3])

    def refresh(ga, gb, sums):
        ga = lax.ppermute(ga, "gx", first_x)
        gb = lax.ppermute(gb, "gx", second_x)
        return ga, gb, gather(sums)

    *state, G, Gs, ga, gb, sums = call(
        first_step, (*states, wide, seam, side, side, rows), flux, 9, {2 + i: i for i in range(6)}
    )(ea, eb, *fields, *seams)
    C, Cs, G, Gs, ga, gb, sums = call(next_step, (wide, seam, wide, seam, side, side, rows), flux, 9)(
        *state, G, Gs, *refresh(ga, gb, sums)
    )
    state = (C, *state[1:3], Cs, *state[4:])
    current, gradient, applied, sums = call(
        last_step, (block, block, block, rows), (wide, seam, wide, seam, *flux), 14
    )(*state, G, Gs, *refresh(ga, gb, sums))
    (updated,) = call(finish, (block,))(current, gradient, gather(sums))
    return updated, applied


def solution(mesh):
    spec = P(None, "gx", "gy", "gz")

    return jax.shard_map(
        local, mesh=mesh, in_specs=(spec, spec, spec), out_specs=(spec, spec), check_vma=False
    )
```

```python
import jax
import jax.numpy as jnp
from jax import lax
from jax.experimental import pallas as pl
from jax.experimental.pallas import tpu as pltpu
from jax.sharding import PartitionSpec as P


ALL = ("gx", "gy", "gz")
F32 = jnp.float32
NX, NY, NZ = 16, 32, 128
DEPTHS = (7, 5, 5)
DX = 3
X_DEPTHS = (DX, 1, 1)
X0, Y0 = DX, 8
XE, YE = NX + 2 * DX, 56
TOP = Y0 + NY
GRID_X, GRID_Y = 256, 128
COUPLE = 0.05 * -2.0 * 0.0625
SLOT, TILES = 16, 4
XY_ROWS, EDGE_ROWS = 44, 128
SEAM_AT = 2 * sum(X_DEPTHS)
SIDE = slice(Y0 - 4, Y0 + NY + 4)
SIDE_ROWS = NY + 8
UNROLL = 4


def lane_ids(rows):
    return lax.broadcasted_iota(jnp.int32, (rows, NZ), 1)


def row_ids(rows):
    return lax.broadcasted_iota(jnp.int32, (rows, NZ), 0)


def own_lanes(rows, iz):
    return (lane_ids(rows) % SLOT) // 8 == iz


def highs(axis):
    first = 1 - lax.axis_index(axis) % 2
    return first, 1 - first


def face_layers():
    return ((0, DX, 0), (1, 1, 2 * DX), (2, 1, 2 * DX + 2))


def xy_pieces():
    row = 0
    for side in range(2):
        for m in range(2):
            for away in (1, 2):
                yield row, 7 - away, side, m, away
                row += 7 - away


def seam_pieces():
    row = XY_ROWS
    for tile in range(TILES):
        for m in range(2):
            for f, count in ((0, 6), (1, 4), (2, 4)) if tile in (1, 2) else ((0, 6),):
                yield row, count, tile, m, f
                row += count


def pack(c, w, t, *refs):
    fields, seams, (ya, yb, z, sems) = refs[:3], refs[3:6], refs[6:]
    iz = lax.axis_index("gz")
    copies = []
    for f, source in enumerate((c, w, t)):
        for m in range(2):
            copy = pltpu.make_async_copy(
                source.at[m],
                fields[f].at[m, pl.ds(X0, NX), pl.ds(Y0, NY)],
                sems.at[2 * f + m],
            )
            copy.start()
            copies.append(copy)
    for copy in copies:
        copy.wait()
    for high, out in zip(highs("gy"), (ya, yb)):
        for m in range(2):
            for x in range(NX):
                row = (m * NX + x) * sum(DEPTHS)
                for f, depth in enumerate(DEPTHS):
                    start = Y0 + high * (NY - depth)
                    out[row : row + depth] = fields[f][m, X0 + x, pl.ds(start, depth)]
                    row += depth
    lane, own = lane_ids(NY), own_lanes(NY, iz)
    swap = 8 + 112 * iz
    for half in range(2):
        targets = []
        for m in range(2):
            packed = []
            for f in range(3):
                acc = jnp.zeros((NY, NZ), F32)
                for s in range(8):
                    block = fields[f][m, X0 + 8 * half + s, Y0:TOP]
                    turned = pltpu.roll(block, (SLOT * s + 8) % NZ, 1)
                    acc = jnp.where(jnp.logical_and(lane // SLOT == s, own), turned, acc)
                seams[f][m, 1 + half, Y0:TOP] = acc
                packed.append(acc)
            z[half, m] = packed[0] + pltpu.roll(packed[1], swap, 1)
            targets.append(packed[2])
        z[half, 2] = targets[0] + pltpu.roll(targets[1], swap, 1)


def clear(*refs):
    fields, seams = refs[6:9], refs[9:12]
    blank = jnp.zeros((YE, NZ), F32)
    for field in fields:
        for m in range(2):
            for x in (*range(X0), *range(X0 + NX, XE)):
                field[m, x] = blank
            for x in range(X0, X0 + NX):
                field[m, x, 0:Y0] = blank[0:Y0]
                field[m, x, TOP:YE] = blank[TOP:YE]
    for seam in seams:
        for m in range(2):
            for tile in (0, 3):
                seam[m, tile] = blank
            for tile in (1, 2):
                seam[m, tile, 0:Y0] = blank[0:Y0]
                seam[m, tile, TOP:YE] = blank[TOP:YE]


def merge(z, C, W, T, *refs):
    fields, seams, outs = (C, W, T), refs[3:6], refs[6:]
    iz = lax.axis_index("gz")
    own = own_lanes(NY, iz)
    swap = 8 + 112 * iz

    def other(tile):
        return pltpu.roll(tile, swap, 1)

    for half in range(2):
        tiles = [z[half, n] for n in range(3)]
        halves = ((tiles[0], tiles[1]), (other(tiles[0]), other(tiles[1])), (tiles[2], other(tiles[2])))
        for f in range(3):
            for m in range(2):
                here = (m, 1 + half, slice(Y0, TOP))
                seams[f][here] = jnp.where(own, seams[f][here], halves[f][m])
    for high, out in zip(highs("gx"), outs):
        for m in range(2):
            for f, depth, at in face_layers():
                start = X0 + high * (NX - depth)
                for layer in range(depth):
                    out[at + 2 * layer + m] = fields[f][m, start + layer, Y0:TOP]
            out[SEAM_AT + m] = seams[0][m, 1 + high, Y0:TOP]


def build(xa, xb, *refs):
    seams, (ea, eb) = refs[3:6], refs[6:]
    lane, own = lane_ids(NY), own_lanes(NY, lax.axis_index("gz"))
    for high, face in zip(highs("gx"), (xa, xb)):
        slot = jnp.where(high == 1, 0, 7)
        near = jnp.logical_and(lane // SLOT == slot, own)
        for m in range(2):
            seams[0][m, 3 * high, Y0:TOP] = face[SEAM_AT + m]
            for f, depth, at in face_layers()[1:]:
                turned = pltpu.roll(face[at + m], (SLOT * slot + 8) % NZ, 1)
                seams[f][m, 3 * high, Y0:TOP] = jnp.where(near, turned, 0.0)
    high_x = highs("gx")
    for high, out in zip(highs("gy"), (ea, eb)):
        for row, count, side, m, away in xy_pieces():
            layer = jnp.where(high_x[side] == 1, away - 1, DX - away)
            start = high * (NY - count)
            out[row : row + count] = (xa, xb)[side][2 * layer + m, pl.ds(start, count)]
        for row, count, tile, m, f in seam_pieces():
            start = Y0 + high * (NY - count)
            out[row : row + count] = seams[f][m, tile, pl.ds(start, count)]
        out[124:128] = jnp.zeros((4, NZ), F32)


def place(xa, xb, ya, yb, *refs):
    fields = refs[3:]
    for high, face in zip(highs("gx"), (xa, xb)):
        for f, depth, at in face_layers():
            start = jnp.where(high == 1, X0 + NX, X0 - depth)
            for layer in range(depth):
                for m in range(2):
                    fields[f][m, start + layer, Y0:TOP] = face[at + 2 * layer + m]
    for high, face in zip(highs("gy"), (ya, yb)):
        for m in range(2):
            for x in range(NX):
                row = (m * NX + x) * sum(DEPTHS)
                for f, depth in enumerate(DEPTHS):
                    start = jnp.where(high == 1, TOP, Y0 - depth)
                    fields[f][m, X0 + x, pl.ds(start, depth)] = face[row : row + depth]
                    row += depth


def place_edges(ea, eb, fields, seams):
    high_x = highs("gx")
    for high, edge in zip(highs("gy"), (ea, eb)):
        for row, count, side, m, away in xy_pieces():
            x = jnp.where(high_x[side] == 1, X0 + NX - 1 + away, X0 - away)
            start = jnp.where(high == 1, TOP, Y0 - count)
            fields[0][m, x, pl.ds(start, count)] = edge[row : row + count]
        for row, count, tile, m, f in seam_pieces():
            start = jnp.where(high == 1, TOP, Y0 - count)
            seams[f][m, tile, pl.ds(start, count)] = edge[row : row + count]


def cross(a, b):
    return (
        a[1] * b[2] - a[2] * b[1],
        a[2] * b[0] - a[0] * b[2],
        a[0] * b[1] - a[1] * b[0],
    )


def beside(own, first, last):
    up = jnp.where(last, 0.0, pltpu.roll(own, NZ - 1, 1))
    return up, jnp.where(first, 0.0, pltpu.roll(own, 1, 1))


class Along:
    def __init__(self):
        iz = lax.axis_index("gz")
        self.iz = iz
        lane = lane_ids(8)
        self.first, self.last = lane == 0, lane == NZ - 1
        self.up_on = (1 - iz).astype(F32)
        self.down_on = iz.astype(F32)

    def slot(self, x):
        place = x - X0 + 8
        return place // 8, (119 + 2 * self.iz + NZ - SLOT * (place % 8)) % NZ

    def __call__(self, own, seam, shift):
        over = pltpu.roll(seam, shift, 1)
        up = jnp.where(self.last, over * self.up_on, pltpu.roll(own, NZ - 1, 1))
        down = jnp.where(self.first, over * self.down_on, pltpu.roll(own, 1, 1))
        return up, down


def seam_x(ref, lead, tile, rows):
    lane = lane_ids(8)
    own = ref[(*lead, tile, rows)]
    after = ref[(*lead, min(tile + 1, TILES - 1), rows)]
    before = ref[(*lead, max(tile - 1, 0), rows)]
    up = jnp.where(lane < NZ - SLOT, pltpu.roll(own, NZ - SLOT, 1), pltpu.roll(after, NZ - SLOT, 1))
    down = jnp.where(lane >= SLOT, pltpu.roll(own, SLOT, 1), pltpu.roll(before, SLOT, 1))
    return own, up, down


def chunks(rows):
    return -(-rows // 8)


def seam_gradients(C, W, T, G, Fl, depth):
    ix, iy = lax.axis_index("gx"), lax.axis_index("gy")
    lane = lane_ids(8)

    def keep(tile, y):
        place = ix * NX + (8 * tile - 8) + lane // SLOT
        row = row_ids(8) + (iy * NY - Y0) + y
        inside = jnp.logical_and(place >= 0, place < GRID_X)
        inside = jnp.logical_and(inside, jnp.logical_and(row >= 0, row < GRID_Y))
        return inside.astype(F32)

    def flux_at(k, carry):
        y = Y0 - depth - 1 + 8 * k
        here = pl.ds(y, 8)
        for tile in range(TILES):
            slope = []
            for m in range(2):
                own, after, before = seam_x(C, (m,), tile, here)
                slope.append(
                    (
                        after - before,
                        C[m, tile, pl.ds(y + 1, 8)] - C[m, tile, pl.ds(y - 1, 8)],
                        pltpu.roll(own, NZ - 1, 1) - pltpu.roll(own, 1, 1),
                    )
                )
            a, b = slope
            inside = keep(tile, y)
            crossed = tuple(inside * v for v in cross(a, b))
            for n, value in enumerate(cross(b, crossed) + cross(crossed, a)):
                Fl[n, tile, here] = value
        return carry

    def gradient_at(k, carry):
        y = Y0 - depth + 8 * k
        here, up, down = pl.ds(y, 8), pl.ds(y + 1, 8), pl.ds(y - 1, 8)
        for tile in range(TILES):
            inside = keep(tile, y)
            for m in range(2):
                n = 3 * m
                own, after, before = seam_x(C, (m,), tile, here)
                near = after + before + C[m, tile, up] + C[m, tile, down]
                near = near + pltpu.roll(own, NZ - 1, 1) + pltpu.roll(own, 1, 1)
                _, after, before = seam_x(Fl, (n,), tile, here)
                along = Fl[n + 2, tile, here]
                spread = after - before + (Fl[n + 1, tile, up] - Fl[n + 1, tile, down])
                spread = spread + (pltpu.roll(along, NZ - 1, 1) - pltpu.roll(along, 1, 1))
                value = W[m, tile, here] * (own - T[m, tile, here])
                value = value + (6.0 * own - near) + COUPLE * spread
                G[m, tile, here] = inside * value
        return carry

    def both_at(k, carry):
        flux_at(k, 0)
        gradient_at(k - 2, 0)
        return carry

    count = chunks(NY + 2 * depth)
    lax.fori_loop(0, 2, flux_at, 0)
    lax.fori_loop(2, count, both_at, 0)
    lax.fori_loop(count - 2, count, gradient_at, 0)


def gradients(fields, seams, G, Gs, Fl, Fs, depth):
    C, W, T = fields
    seam_gradients(*seams, Gs, Fs, depth)
    ix, iy, iz = (lax.axis_index(axis) for axis in ALL)
    lane = lane_ids(8)
    first, last = lane == 0, lane == NZ - 1
    cut = lane - (NZ - 2) * (1 - iz)
    cut = jnp.logical_and(cut >= 0, cut < 2)

    def keep(x, y):
        place = ix * NX + (x - X0)
        inside_x = jnp.logical_and(place >= 0, place < GRID_X).astype(F32)
        row = row_ids(8) + (iy * NY + (y - Y0))
        return jnp.where(jnp.logical_and(row >= 0, row < GRID_Y), inside_x, 0.0)

    def flux_at(x, carry):
        for k in range(chunks(NY + 2 * depth + 2)):
            y = Y0 - depth - 1 + 8 * k
            here, up, down = slice(y, y + 8), slice(y + 1, y + 9), slice(y - 1, y + 7)
            slope, around = [], []
            for m in range(2):
                after, before = beside(C[m, x, here], first, last)
                slope.append(
                    (
                        C[m, x + 1, here] - C[m, x - 1, here],
                        C[m, x, up] - C[m, x, down],
                        after - before,
                    )
                )
                around.append(after + before)
            a, b = slope
            inside = keep(x, y)
            crossed = tuple(inside * v for v in cross(a, b))
            for m, flux in enumerate((cross(b, crossed), cross(crossed, a))):
                after, before = beside(flux[2], first, last)
                Fl[3 * m, x, here] = flux[0]
                Fl[3 * m + 1, x, here] = flux[1]
                Fl[3 * m + 2, x, here] = COUPLE * (after - before) - around[m]
        return carry

    def gradient_at(x, carry):
        place = x - X0 + 8
        tile, shift = place // 8, (120 + NZ - SLOT * (place % 8)) % NZ
        for k in range(chunks(NY + 2 * depth)):
            y = Y0 - depth + 8 * k
            here, up, down = slice(y, y + 8), slice(y + 1, y + 9), slice(y - 1, y + 7)
            inside = keep(x, y)
            for m in range(2):
                n = 3 * m
                own = C[m, x, here]
                near = (C[m, x + 1, here] + C[m, x - 1, here]) + (C[m, x, up] + C[m, x, down])
                spread = Fl[n, x + 1, here] - Fl[n, x - 1, here]
                spread = spread + (Fl[n + 1, x, up] - Fl[n + 1, x, down])
                value = W[m, x, here] * (own - T[m, x, here]) + (6.0 * own - near)
                value = inside * (value + (Fl[n + 2, x, here] + COUPLE * spread))
                G[m, x, here] = jnp.where(cut, pltpu.roll(Gs[m, tile, here], shift, 1), value)
        return carry

    def pair_at(x, fluxes, slopes):
        if fluxes:
            flux_at(x, 0)
            flux_at(x + 1, 0)
        if slopes:
            gradient_at(x - 3, 0)
            gradient_at(x - 2, 0)

    def both_at(i, carry):
        pair_at(X0 - 2 + 2 * i, True, True)
        return carry

    def lead_at(i, carry):
        pair_at(X0 - 2 + 2 * i, True, False)
        return carry

    lax.fori_loop(0, 2, lead_at, 0)
    lax.fori_loop(2, NX // 2 + 2, both_at, 0)
    pair_at(X0 + NX + 2, False, True)


def totals(W, G, Gs, applied, sums):
    along = Along()

    def body(x, carry):
        norm, curve = carry
        tile, shift = along.slot(x)
        for k in range(NY // 8):
            y = Y0 + 8 * k
            here, up, down = slice(y, y + 8), slice(y + 1, y + 9), slice(y - 1, y + 7)
            for m in range(2):
                own = G[m, x, here]
                after, before = along(own, Gs[m, tile, here], shift)
                near = after + G[m, x + 1, here] + G[m, x, up]
                if applied is None:
                    near = near + near
                else:
                    near = near + before + G[m, x - 1, here] + G[m, x, down]
                value = W[m, x, here] * own + (6.0 * own - near)
                if applied is not None:
                    applied[m, x - X0, 8 * k : 8 * k + 8] = value
                norm = norm + own * own
                curve = curve + own * value
        return norm, curve

    zero = jnp.zeros((8, NZ), F32)
    norm, curve = lax.fori_loop(X0, X0 + NX, body, (zero, zero), unroll=UNROLL)
    norm, curve = (jnp.sum(v, axis=0, keepdims=True) for v in (norm, curve))
    row = jnp.where(lane_ids(1) < NZ // 2, norm + pltpu.roll(norm, 64, 1), curve + pltpu.roll(curve, 64, 1))
    row = jnp.broadcast_to(row, (8, NZ))
    for k in range(sums.shape[0] // 8):
        sums[8 * k : 8 * k + 8] = row


def step_of(gathered):
    column = jnp.sum(gathered[...], axis=0, keepdims=True)
    lane = lane_ids(1)
    norm = jnp.sum(jnp.where(lane < NZ // 2, column, 0.0), axis=1, keepdims=True)
    curve = jnp.sum(jnp.where(lane >= NZ // 2, column, 0.0), axis=1, keepdims=True)
    return jnp.broadcast_to(norm, (8, NZ)) / jnp.broadcast_to(curve, (8, NZ))


def sides(G, Gs, ga, gb):
    for high, out in zip(highs("gx"), (ga, gb)):
        for m in range(2):
            for layer in range(DX):
                out[2 * layer + m] = G[m, X0 + high * (NX - DX) + layer, SIDE]
            out[2 * DX + m] = Gs[m, 1 + high, SIDE]


def moved(C, Cs, G, Gs, ga, gb, step, New, News, depth):
    rows = [slice(Y0 - depth + 8 * k, Y0 - depth + 8 * k + 8) for k in range(chunks(NY + 2 * depth))]

    def body(x, carry):
        for here in rows:
            for m in range(2):
                New[m, x, here] = C[m, x, here] - step * G[m, x, here]
        return carry

    lax.fori_loop(X0, X0 + NX, body, 0)
    for tile in (1, 2):
        for here in rows:
            for m in range(2):
                News[m, tile, here] = Cs[m, tile, here] - step * Gs[m, tile, here]
    for high, side in zip(highs("gx"), (ga, gb)):
        for m in range(2):
            for k in range(SIDE_ROWS // 8):
                here, row = slice(SIDE.start + 8 * k, SIDE.start + 8 * k + 8), slice(8 * k, 8 * k + 8)
                for layer in range(DX):
                    x = high * (X0 + NX) + layer
                    New[m, x, here] = C[m, x, here] - step * side[2 * layer + m, row]
                News[m, 3 * high, here] = Cs[m, 3 * high, here] - step * side[2 * DX + m, row]


def first_step(ea, eb, *refs):
    fields, seams, (G, Gs, ga, gb, sums, Fl, Fs) = refs[6:9], refs[9:12], refs[12:]
    place_edges(ea, eb, fields, seams)
    gradients(fields, seams, G, Gs, Fl, Fs, 5)
    sides(G, Gs, ga, gb)
    totals(fields[1], G, Gs, None, sums)


def next_step(C, W, T, Cs, Ws, Ts, G, Gs, ga, gb, gathered, *refs):
    New, News, Gn, Gns, sa, sb, sums, Fl, Fs = refs
    moved(C, Cs, G, Gs, ga, gb, step_of(gathered), New, News, 5)
    gradients((New, W, T), (News, Ws, Ts), Gn, Gns, Fl, Fs, 3)
    sides(Gn, Gns, sa, sb)
    totals(W, Gn, Gns, None, sums)


def last_step(C, W, T, Cs, Ws, Ts, G, Gs, ga, gb, gathered, *refs):
    current, gradient, applied, sums, New, News, Gn, Gns, Fl, Fs = refs
    moved(C, Cs, G, Gs, ga, gb, step_of(gathered), New, News, 3)
    gradients((New, W, T), (News, Ws, Ts), Gn, Gns, Fl, Fs, 1)
    totals(W, Gn, Gns, applied, sums)

    def body(x, carry):
        for m in range(2):
            current[m, x] = New[m, X0 + x, Y0:TOP]
            gradient[m, x] = Gn[m, X0 + x, Y0:TOP]
        return carry

    lax.fori_loop(0, NX, body, 0)


def finish(current, gradient, applied, gathered, updated, applied_out, sem):
    copy = pltpu.make_async_copy(applied, applied_out, sem.at[0])
    copy.start()
    step = step_of(gathered)

    def body(x, carry):
        for m in range(2):
            for k in range(NY // 8):
                here = (m, x, slice(8 * k, 8 * k + 8))
                updated[here] = current[here] - step * gradient[here]
        return carry

    lax.fori_loop(0, NX, body, 0)
    copy.wait()


def call(body, outs, scratch=(), mib=2, alias=None, **more):
    return pl.pallas_call(
        body,
        out_shape=tuple(jax.ShapeDtypeStruct(s, F32) for s in outs),
        scratch_shapes=[pltpu.VMEM(s, F32) if isinstance(s, tuple) else s for s in scratch],
        compiler_params=pltpu.CompilerParams(vmem_limit_bytes=mib * 1024 * 1024),
        input_output_aliases=alias or {},
        **more,
    )


def pairs_of(size):
    first = [(i, i ^ 1) for i in range(size)]
    second = [(i, i - 1 if i % 2 == 0 else i + 1) for i in range(1, size - 1)]
    return first, second


def gather(sums):
    return lax.all_to_all(sums, ALL, 0, 0, tiled=True)


def local(models, targets, weights):
    nx, ny = lax.axis_size("gx"), lax.axis_size("gy")
    block = (2, NX, NY, NZ)
    wide, seam = (2, XE, YE, NZ), (2, TILES, YE, NZ)
    flux = ((6, XE, YE, NZ), (6, TILES, YE, NZ))
    rows = (nx * ny * 2, NZ)
    states = (wide,) * 3 + (seam,) * 3
    x_face, y_face = (SEAM_AT + 2, NY, NZ), (2 * NX * sum(DEPTHS), NZ)
    edge, side = (EDGE_ROWS, NZ), (2 * DX + 2, SIDE_ROWS, NZ)
    *state, ya, yb, z = call(
        pack,
        (*states, y_face, y_face, (2, 3, NY, NZ)),
        (pltpu.SemaphoreType.DMA((6,)),),
        in_specs=[pl.BlockSpec(memory_space=pltpu.HBM)] * 3,
    )(models, weights, targets)
    first_x, second_x = pairs_of(nx)
    first_y, second_y = pairs_of(ny)
    z = lax.ppermute(z, "gz", [(0, 1), (1, 0)])
    ya = lax.ppermute(ya, "gy", first_y)
    *seams, xa, xb = call(merge, (seam,) * 3 + (x_face, x_face), alias={4: 0, 5: 1, 6: 2})(z, *state)
    xa, xb = lax.ppermute(xa, "gx", first_x), lax.ppermute(xb, "gx", second_x)
    yb = lax.ppermute(yb, "gy", second_y)
    state = call(clear, states, alias={i: i for i in range(6)})(*state[:3], *seams)
    *seams, ea, eb = call(build, (seam,) * 3 + (edge, edge), alias={2: 0, 3: 1, 4: 2})(
        xa, xb, *state[3:]
    )
    ea, eb = lax.ppermute(ea, "gy", first_y), lax.ppermute(eb, "gy", second_y)
    fields = call(place, (wide,) * 3, alias={4: 0, 5: 1, 6: 2})(xa, xb, ya, yb, *state[:3])

    def refresh(ga, gb, sums):
        ga = lax.ppermute(ga, "gx", first_x)
        gb = lax.ppermute(gb, "gx", second_x)
        return ga, gb, gather(sums)

    *state, G, Gs, ga, gb, sums = call(
        first_step, (*states, wide, seam, side, side, rows), flux, 9, {2 + i: i for i in range(6)}
    )(ea, eb, *fields, *seams)
    C, Cs, G, Gs, ga, gb, sums = call(next_step, (wide, seam, wide, seam, side, side, rows), flux, 9)(
        *state, G, Gs, *refresh(ga, gb, sums)
    )
    state = (C, *state[1:3], Cs, *state[4:])
    current, gradient, applied, sums = call(
        last_step, (block, block, block, rows), (wide, seam, wide, seam, *flux), 14
    )(*state, G, Gs, *refresh(ga, gb, sums))
    return call(
        finish,
        (block, block),
        (pltpu.SemaphoreType.DMA((1,)),),
        out_specs=(pl.BlockSpec(memory_space=pltpu.VMEM), pl.BlockSpec(memory_space=pltpu.HBM)),
    )(current, gradient, applied, gather(sums))


def solution(mesh):
    spec = P(None, "gx", "gy", "gz")

    return jax.shard_map(
        local, mesh=mesh, in_specs=(spec, spec, spec), out_specs=(spec, spec), check_vma=False
    )
```

```python
import jax
import jax.numpy as jnp
from jax import lax
from jax.experimental import pallas as pl
from jax.experimental.pallas import tpu as pltpu
from jax.sharding import PartitionSpec as P


ALL = ("gx", "gy", "gz")
F32 = jnp.float32
NX, NY, NZ = 16, 32, 128
DEPTHS = (7, 5, 5)
DX = 3
X_DEPTHS = (DX, 1, 1)
X0, Y0 = DX, 8
XE, YE = NX + 2 * DX, 56
TOP = Y0 + NY
GRID_X, GRID_Y = 256, 128
COUPLE = 0.05 * -2.0 * 0.0625
SLOT, TILES = 16, 4
XY_ROWS, EDGE_ROWS = 44, 128
SEAM_AT = 2 * sum(X_DEPTHS)
SIDE = slice(Y0 - 4, Y0 + NY + 4)
SIDE_ROWS = NY + 8
UNROLL = 4


def lane_ids(rows):
    return lax.broadcasted_iota(jnp.int32, (rows, NZ), 1)


def row_ids(rows):
    return lax.broadcasted_iota(jnp.int32, (rows, NZ), 0)


def own_lanes(rows, iz):
    return (lane_ids(rows) % SLOT) // 8 == iz


def highs(axis):
    first = 1 - lax.axis_index(axis) % 2
    return first, 1 - first


def face_layers():
    return ((0, DX, 0), (1, 1, 2 * DX), (2, 1, 2 * DX + 2))


def xy_pieces():
    row = 0
    for side in range(2):
        for m in range(2):
            for away in (1, 2):
                yield row, 7 - away, side, m, away
                row += 7 - away


def seam_pieces():
    row = XY_ROWS
    for tile in range(TILES):
        for m in range(2):
            for f, count in ((0, 6), (1, 4), (2, 4)) if tile in (1, 2) else ((0, 6),):
                yield row, count, tile, m, f
                row += count


def pack(c, w, t, *refs):
    fields, seams, (ya, yb, z, sems) = refs[:3], refs[3:6], refs[6:]
    iz = lax.axis_index("gz")
    copies = []
    for f, source in enumerate((c, w, t)):
        for m in range(2):
            copy = pltpu.make_async_copy(
                source.at[m],
                fields[f].at[m, pl.ds(X0, NX), pl.ds(Y0, NY)],
                sems.at[2 * f + m],
            )
            copy.start()
            copies.append(copy)
    for copy in copies:
        copy.wait()
    for high, out in zip(highs("gy"), (ya, yb)):
        for m in range(2):
            for x in range(NX):
                row = (m * NX + x) * sum(DEPTHS)
                for f, depth in enumerate(DEPTHS):
                    start = Y0 + high * (NY - depth)
                    out[row : row + depth] = fields[f][m, X0 + x, pl.ds(start, depth)]
                    row += depth
    lane, own = lane_ids(NY), own_lanes(NY, iz)
    swap = 8 + 112 * iz
    for half in range(2):
        targets = []
        for m in range(2):
            packed = []
            for f in range(3):
                acc = jnp.zeros((NY, NZ), F32)
                for s in range(8):
                    block = fields[f][m, X0 + 8 * half + s, Y0:TOP]
                    turned = pltpu.roll(block, (SLOT * s + 8) % NZ, 1)
                    acc = jnp.where(jnp.logical_and(lane // SLOT == s, own), turned, acc)
                seams[f][m, 1 + half, Y0:TOP] = acc
                packed.append(acc)
            z[half, m] = packed[0] + pltpu.roll(packed[1], swap, 1)
            targets.append(packed[2])
        z[half, 2] = targets[0] + pltpu.roll(targets[1], swap, 1)


def clear(*refs):
    fields, seams = refs[6:9], refs[9:12]
    blank = jnp.zeros((YE, NZ), F32)
    for field in fields:
        for m in range(2):
            for x in (*range(X0), *range(X0 + NX, XE)):
                field[m, x] = blank
            for x in range(X0, X0 + NX):
                field[m, x, 0:Y0] = blank[0:Y0]
                field[m, x, TOP:YE] = blank[TOP:YE]
    for seam in seams:
        for m in range(2):
            for tile in (0, 3):
                seam[m, tile] = blank
            for tile in (1, 2):
                seam[m, tile, 0:Y0] = blank[0:Y0]
                seam[m, tile, TOP:YE] = blank[TOP:YE]


def merge(z, C, W, T, *refs):
    fields, seams, outs = (C, W, T), refs[3:6], refs[6:]
    iz = lax.axis_index("gz")
    own = own_lanes(NY, iz)
    swap = 8 + 112 * iz

    def other(tile):
        return pltpu.roll(tile, swap, 1)

    for half in range(2):
        tiles = [z[half, n] for n in range(3)]
        halves = ((tiles[0], tiles[1]), (other(tiles[0]), other(tiles[1])), (tiles[2], other(tiles[2])))
        for f in range(3):
            for m in range(2):
                here = (m, 1 + half, slice(Y0, TOP))
                seams[f][here] = jnp.where(own, seams[f][here], halves[f][m])
    for high, out in zip(highs("gx"), outs):
        for m in range(2):
            for f, depth, at in face_layers():
                start = X0 + high * (NX - depth)
                for layer in range(depth):
                    out[at + 2 * layer + m] = fields[f][m, start + layer, Y0:TOP]
        near = lane_ids(NY) // (NZ // 2) == high
        both = [seams[0][m, 1 + high, Y0:TOP] for m in range(2)]
        out[SEAM_AT] = jnp.where(near, both[0], pltpu.roll(both[1], NZ // 2, 1))


def build(xa, xb, *refs):
    seams, (ea, eb) = refs[3:6], refs[6:]
    lane, own = lane_ids(NY), own_lanes(NY, lax.axis_index("gz"))
    for high, face in zip(highs("gx"), (xa, xb)):
        slot = jnp.where(high == 1, 0, 7)
        near = jnp.logical_and(lane // SLOT == slot, own)
        for m in range(2):
            seams[0][m, 3 * high, Y0:TOP] = face[SEAM_AT] if m == 0 else pltpu.roll(face[SEAM_AT], NZ // 2, 1)
            for f, depth, at in face_layers()[1:]:
                turned = pltpu.roll(face[at + m], (SLOT * slot + 8) % NZ, 1)
                seams[f][m, 3 * high, Y0:TOP] = jnp.where(near, turned, 0.0)
    high_x = highs("gx")
    for high, out in zip(highs("gy"), (ea, eb)):
        for row, count, side, m, away in xy_pieces():
            layer = jnp.where(high_x[side] == 1, away - 1, DX - away)
            start = high * (NY - count)
            out[row : row + count] = (xa, xb)[side][2 * layer + m, pl.ds(start, count)]
        for row, count, tile, m, f in seam_pieces():
            start = Y0 + high * (NY - count)
            out[row : row + count] = seams[f][m, tile, pl.ds(start, count)]
        out[124:128] = jnp.zeros((4, NZ), F32)


def place(xa, xb, ya, yb, *refs):
    fields = refs[3:]
    for high, face in zip(highs("gx"), (xa, xb)):
        for f, depth, at in face_layers():
            start = jnp.where(high == 1, X0 + NX, X0 - depth)
            for layer in range(depth):
                for m in range(2):
                    fields[f][m, start + layer, Y0:TOP] = face[at + 2 * layer + m]
    for high, face in zip(highs("gy"), (ya, yb)):
        for m in range(2):
            for x in range(NX):
                row = (m * NX + x) * sum(DEPTHS)
                for f, depth in enumerate(DEPTHS):
                    start = jnp.where(high == 1, TOP, Y0 - depth)
                    fields[f][m, X0 + x, pl.ds(start, depth)] = face[row : row + depth]
                    row += depth


def place_edges(ea, eb, fields, seams):
    high_x = highs("gx")
    for high, edge in zip(highs("gy"), (ea, eb)):
        for row, count, side, m, away in xy_pieces():
            x = jnp.where(high_x[side] == 1, X0 + NX - 1 + away, X0 - away)
            start = jnp.where(high == 1, TOP, Y0 - count)
            fields[0][m, x, pl.ds(start, count)] = edge[row : row + count]
        for row, count, tile, m, f in seam_pieces():
            start = jnp.where(high == 1, TOP, Y0 - count)
            seams[f][m, tile, pl.ds(start, count)] = edge[row : row + count]


def cross(a, b):
    return (
        a[1] * b[2] - a[2] * b[1],
        a[2] * b[0] - a[0] * b[2],
        a[0] * b[1] - a[1] * b[0],
    )


def beside(own, first, last):
    up = jnp.where(last, 0.0, pltpu.roll(own, NZ - 1, 1))
    return up, jnp.where(first, 0.0, pltpu.roll(own, 1, 1))


class Along:
    def __init__(self):
        iz = lax.axis_index("gz")
        self.iz = iz
        lane = lane_ids(8)
        self.first, self.last = lane == 0, lane == NZ - 1
        self.up_on = (1 - iz).astype(F32)
        self.down_on = iz.astype(F32)

    def slot(self, x):
        place = x - X0 + 8
        return place // 8, (119 + 2 * self.iz + NZ - SLOT * (place % 8)) % NZ

    def __call__(self, own, seam, shift):
        over = pltpu.roll(seam, shift, 1)
        up = jnp.where(self.last, over * self.up_on, pltpu.roll(own, NZ - 1, 1))
        down = jnp.where(self.first, over * self.down_on, pltpu.roll(own, 1, 1))
        return up, down


def seam_x(ref, lead, tile, rows):
    lane = lane_ids(8)
    own = ref[(*lead, tile, rows)]
    after = ref[(*lead, min(tile + 1, TILES - 1), rows)]
    before = ref[(*lead, max(tile - 1, 0), rows)]
    up = jnp.where(lane < NZ - SLOT, pltpu.roll(own, NZ - SLOT, 1), pltpu.roll(after, NZ - SLOT, 1))
    down = jnp.where(lane >= SLOT, pltpu.roll(own, SLOT, 1), pltpu.roll(before, SLOT, 1))
    return own, up, down


def chunks(rows):
    return -(-rows // 8)


def seam_gradients(C, W, T, G, Fl, depth):
    ix, iy = lax.axis_index("gx"), lax.axis_index("gy")
    lane = lane_ids(8)

    def keep(tile, y):
        place = ix * NX + (8 * tile - 8) + lane // SLOT
        row = row_ids(8) + (iy * NY - Y0) + y
        inside = jnp.logical_and(place >= 0, place < GRID_X)
        inside = jnp.logical_and(inside, jnp.logical_and(row >= 0, row < GRID_Y))
        return inside.astype(F32)

    def flux_at(k, carry):
        y = Y0 - depth - 1 + 8 * k
        here = pl.ds(y, 8)
        for tile in range(TILES):
            slope = []
            for m in range(2):
                own, after, before = seam_x(C, (m,), tile, here)
                slope.append(
                    (
                        after - before,
                        C[m, tile, pl.ds(y + 1, 8)] - C[m, tile, pl.ds(y - 1, 8)],
                        pltpu.roll(own, NZ - 1, 1) - pltpu.roll(own, 1, 1),
                    )
                )
            a, b = slope
            inside = keep(tile, y)
            crossed = tuple(inside * v for v in cross(a, b))
            for n, value in enumerate(cross(b, crossed) + cross(crossed, a)):
                Fl[n, tile, here] = value
        return carry

    def gradient_at(k, carry):
        y = Y0 - depth + 8 * k
        here, up, down = pl.ds(y, 8), pl.ds(y + 1, 8), pl.ds(y - 1, 8)
        for tile in range(TILES):
            inside = keep(tile, y)
            for m in range(2):
                n = 3 * m
                own, after, before = seam_x(C, (m,), tile, here)
                near = after + before + C[m, tile, up] + C[m, tile, down]
                near = near + pltpu.roll(own, NZ - 1, 1) + pltpu.roll(own, 1, 1)
                _, after, before = seam_x(Fl, (n,), tile, here)
                along = Fl[n + 2, tile, here]
                spread = after - before + (Fl[n + 1, tile, up] - Fl[n + 1, tile, down])
                spread = spread + (pltpu.roll(along, NZ - 1, 1) - pltpu.roll(along, 1, 1))
                value = W[m, tile, here] * (own - T[m, tile, here])
                value = value + (6.0 * own - near) + COUPLE * spread
                G[m, tile, here] = inside * value
        return carry

    def both_at(k, carry):
        flux_at(k, 0)
        gradient_at(k - 2, 0)
        return carry

    count = chunks(NY + 2 * depth)
    lax.fori_loop(0, 2, flux_at, 0)
    lax.fori_loop(2, count, both_at, 0)
    lax.fori_loop(count - 2, count, gradient_at, 0)


def gradients(fields, seams, G, Gs, Fl, Fs, depth):
    C, W, T = fields
    seam_gradients(*seams, Gs, Fs, depth)
    ix, iy, iz = (lax.axis_index(axis) for axis in ALL)
    lane = lane_ids(8)
    first, last = lane == 0, lane == NZ - 1
    cut = lane - (NZ - 2) * (1 - iz)
    cut = jnp.logical_and(cut >= 0, cut < 2)

    def keep(x, y):
        place = ix * NX + (x - X0)
        inside_x = jnp.logical_and(place >= 0, place < GRID_X).astype(F32)
        row = row_ids(8) + (iy * NY + (y - Y0))
        return jnp.where(jnp.logical_and(row >= 0, row < GRID_Y), inside_x, 0.0)

    def flux_at(x, carry):
        for k in range(chunks(NY + 2 * depth + 2)):
            y = Y0 - depth - 1 + 8 * k
            here, up, down = slice(y, y + 8), slice(y + 1, y + 9), slice(y - 1, y + 7)
            slope, around = [], []
            for m in range(2):
                after, before = beside(C[m, x, here], first, last)
                slope.append(
                    (
                        C[m, x + 1, here] - C[m, x - 1, here],
                        C[m, x, up] - C[m, x, down],
                        after - before,
                    )
                )
                around.append(after + before)
            a, b = slope
            inside = keep(x, y)
            crossed = tuple(inside * v for v in cross(a, b))
            for m, flux in enumerate((cross(b, crossed), cross(crossed, a))):
                after, before = beside(flux[2], first, last)
                Fl[3 * m, x, here] = flux[0]
                Fl[3 * m + 1, x, here] = flux[1]
                Fl[3 * m + 2, x, here] = COUPLE * (after - before) - around[m]
        return carry

    def gradient_at(x, carry):
        place = x - X0 + 8
        tile, shift = place // 8, (120 + NZ - SLOT * (place % 8)) % NZ
        for k in range(chunks(NY + 2 * depth)):
            y = Y0 - depth + 8 * k
            here, up, down = slice(y, y + 8), slice(y + 1, y + 9), slice(y - 1, y + 7)
            inside = keep(x, y)
            for m in range(2):
                n = 3 * m
                own = C[m, x, here]
                near = (C[m, x + 1, here] + C[m, x - 1, here]) + (C[m, x, up] + C[m, x, down])
                spread = Fl[n, x + 1, here] - Fl[n, x - 1, here]
                spread = spread + (Fl[n + 1, x, up] - Fl[n + 1, x, down])
                value = W[m, x, here] * (own - T[m, x, here]) + (6.0 * own - near)
                value = inside * (value + (Fl[n + 2, x, here] + COUPLE * spread))
                G[m, x, here] = jnp.where(cut, pltpu.roll(Gs[m, tile, here], shift, 1), value)
        return carry

    def pair_at(x, fluxes, slopes):
        if fluxes:
            flux_at(x, 0)
            flux_at(x + 1, 0)
        if slopes:
            gradient_at(x - 3, 0)
            gradient_at(x - 2, 0)

    def both_at(i, carry):
        pair_at(X0 - 2 + 2 * i, True, True)
        return carry

    def lead_at(i, carry):
        pair_at(X0 - 2 + 2 * i, True, False)
        return carry

    lax.fori_loop(0, 2, lead_at, 0)
    lax.fori_loop(2, NX // 2 + 2, both_at, 0)
    pair_at(X0 + NX + 2, False, True)


def totals(W, G, Gs, applied, sums):
    along = Along()

    def body(x, carry):
        norm, curve = carry
        tile, shift = along.slot(x)
        for k in range(NY // 8):
            y = Y0 + 8 * k
            here, up, down = slice(y, y + 8), slice(y + 1, y + 9), slice(y - 1, y + 7)
            for m in range(2):
                own = G[m, x, here]
                after, before = along(own, Gs[m, tile, here], shift)
                near = after + G[m, x + 1, here] + G[m, x, up]
                if applied is None:
                    near = near + near
                else:
                    near = near + before + G[m, x - 1, here] + G[m, x, down]
                value = W[m, x, here] * own + (6.0 * own - near)
                if applied is not None:
                    applied[m, x - X0, 8 * k : 8 * k + 8] = value
                norm = norm + own * own
                curve = curve + own * value
        return norm, curve

    zero = jnp.zeros((8, NZ), F32)
    norm, curve = lax.fori_loop(X0, X0 + NX, body, (zero, zero), unroll=UNROLL)
    norm, curve = (jnp.sum(v, axis=0, keepdims=True) for v in (norm, curve))
    row = jnp.where(lane_ids(1) < NZ // 2, norm + pltpu.roll(norm, 64, 1), curve + pltpu.roll(curve, 64, 1))
    row = jnp.broadcast_to(row, (8, NZ))
    for k in range(sums.shape[0] // 8):
        sums[8 * k : 8 * k + 8] = row


def step_of(gathered):
    column = jnp.sum(gathered[...], axis=0, keepdims=True)
    lane = lane_ids(1)
    norm = jnp.sum(jnp.where(lane < NZ // 2, column, 0.0), axis=1, keepdims=True)
    curve = jnp.sum(jnp.where(lane >= NZ // 2, column, 0.0), axis=1, keepdims=True)
    return jnp.broadcast_to(norm, (8, NZ)) / jnp.broadcast_to(curve, (8, NZ))


def sides(G, Gs, ga, gb):
    for high, out in zip(highs("gx"), (ga, gb)):
        for m in range(2):
            for layer in range(DX):
                out[2 * layer + m] = G[m, X0 + high * (NX - DX) + layer, SIDE]
            out[2 * DX + m] = Gs[m, 1 + high, SIDE]


def moved(C, Cs, G, Gs, ga, gb, step, New, News, depth):
    rows = [slice(Y0 - depth + 8 * k, Y0 - depth + 8 * k + 8) for k in range(chunks(NY + 2 * depth))]

    def body(x, carry):
        for here in rows:
            for m in range(2):
                New[m, x, here] = C[m, x, here] - step * G[m, x, here]
        return carry

    lax.fori_loop(X0, X0 + NX, body, 0)
    for tile in (1, 2):
        for here in rows:
            for m in range(2):
                News[m, tile, here] = Cs[m, tile, here] - step * Gs[m, tile, here]
    for high, side in zip(highs("gx"), (ga, gb)):
        for m in range(2):
            for k in range(SIDE_ROWS // 8):
                here, row = slice(SIDE.start + 8 * k, SIDE.start + 8 * k + 8), slice(8 * k, 8 * k + 8)
                for layer in range(DX):
                    x = high * (X0 + NX) + layer
                    New[m, x, here] = C[m, x, here] - step * side[2 * layer + m, row]
                News[m, 3 * high, here] = Cs[m, 3 * high, here] - step * side[2 * DX + m, row]


def first_step(ea, eb, *refs):
    fields, seams, (G, Gs, ga, gb, sums, Fl, Fs) = refs[6:9], refs[9:12], refs[12:]
    place_edges(ea, eb, fields, seams)
    gradients(fields, seams, G, Gs, Fl, Fs, 5)
    sides(G, Gs, ga, gb)
    totals(fields[1], G, Gs, None, sums)


def next_step(C, W, T, Cs, Ws, Ts, G, Gs, ga, gb, gathered, *refs):
    New, News, Gn, Gns, sa, sb, sums, Fl, Fs = refs
    moved(C, Cs, G, Gs, ga, gb, step_of(gathered), New, News, 5)
    gradients((New, W, T), (News, Ws, Ts), Gn, Gns, Fl, Fs, 3)
    sides(Gn, Gns, sa, sb)
    totals(W, Gn, Gns, None, sums)


def last_step(C, W, T, Cs, Ws, Ts, G, Gs, ga, gb, gathered, *refs):
    current, gradient, applied, sums, New, News, Gn, Gns, Fl, Fs = refs
    moved(C, Cs, G, Gs, ga, gb, step_of(gathered), New, News, 3)
    gradients((New, W, T), (News, Ws, Ts), Gn, Gns, Fl, Fs, 1)
    totals(W, Gn, Gns, applied, sums)

    def body(x, carry):
        for m in range(2):
            current[m, x] = New[m, X0 + x, Y0:TOP]
            gradient[m, x] = Gn[m, X0 + x, Y0:TOP]
        return carry

    lax.fori_loop(0, NX, body, 0)


def finish(current, gradient, applied, gathered, updated, applied_out, sem):
    copy = pltpu.make_async_copy(applied, applied_out, sem.at[0])
    copy.start()
    step = step_of(gathered)

    def body(x, carry):
        for m in range(2):
            for k in range(NY // 8):
                here = (m, x, slice(8 * k, 8 * k + 8))
                updated[here] = current[here] - step * gradient[here]
        return carry

    lax.fori_loop(0, NX, body, 0)
    copy.wait()


def call(body, outs, scratch=(), mib=2, alias=None, **more):
    return pl.pallas_call(
        body,
        out_shape=tuple(jax.ShapeDtypeStruct(s, F32) for s in outs),
        scratch_shapes=[pltpu.VMEM(s, F32) if isinstance(s, tuple) else s for s in scratch],
        compiler_params=pltpu.CompilerParams(vmem_limit_bytes=mib * 1024 * 1024),
        input_output_aliases=alias or {},
        **more,
    )


def pairs_of(size):
    first = [(i, i ^ 1) for i in range(size)]
    second = [(i, i - 1 if i % 2 == 0 else i + 1) for i in range(1, size - 1)]
    return first, second


def gather(sums):
    return lax.all_to_all(sums, ALL, 0, 0, tiled=True)


def local(models, targets, weights):
    nx, ny = lax.axis_size("gx"), lax.axis_size("gy")
    block = (2, NX, NY, NZ)
    wide, seam = (2, XE, YE, NZ), (2, TILES, YE, NZ)
    flux = ((6, XE, YE, NZ), (6, TILES, YE, NZ))
    rows = (nx * ny * 2, NZ)
    states = (wide,) * 3 + (seam,) * 3
    x_face, y_face = (SEAM_AT + 1, NY, NZ), (2 * NX * sum(DEPTHS), NZ)
    edge, side = (EDGE_ROWS, NZ), (2 * DX + 2, SIDE_ROWS, NZ)
    *state, ya, yb, z = call(
        pack,
        (*states, y_face, y_face, (2, 3, NY, NZ)),
        (pltpu.SemaphoreType.DMA((6,)),),
        in_specs=[pl.BlockSpec(memory_space=pltpu.HBM)] * 3,
    )(models, weights, targets)
    first_x, second_x = pairs_of(nx)
    first_y, second_y = pairs_of(ny)
    z = lax.ppermute(z, "gz", [(0, 1), (1, 0)])
    ya = lax.ppermute(ya, "gy", first_y)
    *seams, xa, xb = call(merge, (seam,) * 3 + (x_face, x_face), alias={4: 0, 5: 1, 6: 2})(z, *state)
    xa, xb = lax.ppermute(xa, "gx", first_x), lax.ppermute(xb, "gx", second_x)
    yb = lax.ppermute(yb, "gy", second_y)
    state = call(clear, states, alias={i: i for i in range(6)})(*state[:3], *seams)
    *seams, ea, eb = call(build, (seam,) * 3 + (edge, edge), alias={2: 0, 3: 1, 4: 2})(
        xa, xb, *state[3:]
    )
    ea, eb = lax.ppermute(ea, "gy", first_y), lax.ppermute(eb, "gy", second_y)
    fields = call(place, (wide,) * 3, alias={4: 0, 5: 1, 6: 2})(xa, xb, ya, yb, *state[:3])

    def refresh(ga, gb, sums):
        ga = lax.ppermute(ga, "gx", first_x)
        gb = lax.ppermute(gb, "gx", second_x)
        return ga, gb, gather(sums)

    *state, G, Gs, ga, gb, sums = call(
        first_step, (*states, wide, seam, side, side, rows), flux, 9, {2 + i: i for i in range(6)}
    )(ea, eb, *fields, *seams)
    C, Cs, G, Gs, ga, gb, sums = call(next_step, (wide, seam, wide, seam, side, side, rows), flux, 9)(
        *state, G, Gs, *refresh(ga, gb, sums)
    )
    state = (C, *state[1:3], Cs, *state[4:])
    current, gradient, applied, sums = call(
        last_step, (block, block, block, rows), (wide, seam, wide, seam, *flux), 14
    )(*state, G, Gs, *refresh(ga, gb, sums))
    return call(
        finish,
        (block, block),
        (pltpu.SemaphoreType.DMA((1,)),),
        out_specs=(pl.BlockSpec(memory_space=pltpu.VMEM), pl.BlockSpec(memory_space=pltpu.HBM)),
    )(current, gradient, applied, gather(sums))


def solution(mesh):
    spec = P(None, "gx", "gy", "gz")

    return jax.shard_map(
        local, mesh=mesh, in_specs=(spec, spec, spec), out_specs=(spec, spec), check_vma=False
    )
```
